256 devices in a mesh: occ: 32 (over x, z_lo, core), aux: 8 (over y, z_hi).
Axes of the slice: x: 4, y: 4, z: 8 (z_hi: 2, z_lo: 4; z = z_hi * 4 + z_lo), core: 2. Of those that a mesh axis runs over, the one named last changes fastest.
Arguments:
- b_factors: bfloat16 [32, 256, 12288], P('occ', None, 'aux'), may hold values from -0.056884766 to 0.056884766
- occ_energies: float32 [32], P('occ'), may hold values from -1.2 to -0.3
- vir_energies: float32 [256], replicated, may hold values from 0.1 to 4
- pair_list: int32 [32, 48, 3], P('occ'), may hold values from -1 to 31, as said below
- pair_count: int32 [32], P('occ'), may hold values from 1 to 48, as said below
Outputs:
- pair_energy: float32 [32, 48], P('occ', 'aux')
- total_energy: float32 [], replicated
The draws below stay inside these ranges and needn't reach their ends.
Inputs may be any that keep to these rules, and one draw needn't show every extreme that they name: `pair_list`: row i lists pair_count[i] distinct items (j, a-block, b-block) with j in 0 to 31 and blocks in 0 to 1, ordered by j, then a-block, then b-block; its other slots hold -1 in all three fields. `pair_count`: some occupied orbital lists exactly 48 items.
All inputs are finite; a program needn't handle non-finite values.
Results may differ from the reference program's by a relative error of at most 0.0003.
Values may be sent and summed in bfloat16 or wider, within the bound.
A program may use at most 128 MiB of HBM per device.

```python
import math
import jax
import jax.numpy as jnp
from jax import lax

NAUX = 12288
VB = 128
NVB = 2
MAXP = 48
NV = 256
NOCC = 32


def screened_lists(key):
    base_key = jax.random.fold_in(key, 7)
    count_key, full_key, order_key = jax.random.split(base_key, 3)
    lowest = max(MAXP // 2, 1)
    counts = jax.random.randint(count_key, (NOCC,), lowest, MAXP + 1)
    busiest = jax.random.randint(full_key, (), 0, NOCC)
    counts = counts.at[busiest].set(MAXP)
    candidates = NOCC * NVB * NVB

    def choose(order_seed):
        return jax.random.permutation(order_seed, candidates)[:MAXP]
    chosen = jax.vmap(choose)(jax.random.split(order_key, NOCC))
    slot_index = jnp.arange(MAXP, dtype=jnp.int32)
    live_slots = slot_index[None, :] < counts[:, None]
    codes = jnp.sort(jnp.where(live_slots, chosen, candidates), axis=1)
    partner_ids = jnp.where(live_slots, codes // (NVB * NVB), -1)
    left_blocks = jnp.where(live_slots, codes // NVB % NVB, -1)
    right_blocks = jnp.where(live_slots, codes % NVB, -1)
    table = jnp.stack([partner_ids, left_blocks, right_blocks], axis=-1)
    return (table.astype(jnp.int32), counts.astype(jnp.int32))


def draw_pair_list(key, part):
    return screened_lists(key)[0]


def draw_pair_count(key, part):
    return screened_lists(key)[1]


def levels(stream_key, shape, cuts, low, top_value):
    gain = 1.0
    for axis_at, shards_of in cuts:
        heights = jax.random.uniform(jax.random.fold_in(jax.random.fold_in(stream_key, 6), axis_at), (shards_of,), jnp.float32, low / len(cuts), top_value / len(cuts))
        gain = gain * jnp.repeat(jnp.exp(heights), shape[axis_at] // shards_of).reshape((-1,) + (1,) * (len(shape) - 1 - axis_at))
    return gain


def normal_values(stream_key, dims, width, reach, cuts=(), kind=jnp.bfloat16):
    values = width * jax.random.normal(stream_key, dims, jnp.float32)
    if cuts:
        values = values * levels(stream_key, dims, cuts, -0.22, 0.18)
    return jnp.clip(values, -reach, reach).astype(kind)


def setup_inputs(seed: int = 0) -> dict:
    streams_of = jax.random.split(jax.random.key(seed), 6)
    b_factors = normal_values(streams_of[0], (NOCC, NV, NAUX), 0.0095, 0.056884766, ((0, 32), (2, 8)))
    occ_energies = jnp.clip(-1.2 + 0.90000004 * jax.random.uniform(streams_of[1], (NOCC,), jnp.float32) ** levels(streams_of[1], (NOCC,), ((0, 32),), -0.2, 0.2), -1.2, -0.3)
    vir_energies = jnp.clip(jnp.exp(jax.random.uniform(streams_of[2], (NV,), jnp.float32, math.log(0.1), math.log(4.0))), 0.1, 4.0)
    pair_list = draw_pair_list(jax.random.fold_in(streams_of[5], 71), 0)
    pair_count = draw_pair_count(jax.random.fold_in(streams_of[5], 71), 0)
    return dict(b_factors=b_factors, occ_energies=occ_energies, vir_energies=vir_energies, pair_list=pair_list, pair_count=pair_count)


def reference(b_factors, occ_energies, vir_energies, pair_list, pair_count):
    float_factors = b_factors.astype(jnp.float32)

    def one_orbital(packed):
        orbital, entries, listed = packed
        home_panel = lax.dynamic_index_in_dim(float_factors, orbital, 0, keepdims=False)
        home_energy = lax.dynamic_index_in_dim(occ_energies, orbital, 0, keepdims=False)

        def one_item(packed_item):
            slot_index, entry_row = packed_item
            partner_id = jnp.maximum(entry_row[0], 0).astype(jnp.int32)
            left_block = jnp.maximum(entry_row[1], 0).astype(jnp.int32)
            right_block = jnp.maximum(entry_row[2], 0).astype(jnp.int32)
            partner_panel = lax.dynamic_index_in_dim(float_factors, partner_id, 0, keepdims=False)
            home_left = lax.dynamic_slice_in_dim(home_panel, left_block * VB, VB, 0)
            home_right = lax.dynamic_slice_in_dim(home_panel, right_block * VB, VB, 0)
            partner_left = lax.dynamic_slice_in_dim(partner_panel, left_block * VB, VB, 0)
            partner_right = lax.dynamic_slice_in_dim(partner_panel, right_block * VB, VB, 0)
            direct = jnp.dot(home_left, partner_right.T, precision=lax.Precision.HIGHEST)
            swapped = jnp.dot(home_right, partner_left.T, precision=lax.Precision.HIGHEST)
            left_energy = lax.dynamic_slice_in_dim(vir_energies, left_block * VB, VB, 0)
            right_energy = lax.dynamic_slice_in_dim(vir_energies, right_block * VB, VB, 0)
            partner_energy = lax.dynamic_index_in_dim(occ_energies, partner_id, 0, keepdims=False)
            denominator = (left_energy[:, None] + right_energy[None, :]) - home_energy - partner_energy
            energy = -jnp.sum(direct * (2.0 * direct - swapped.T) / denominator)
            return jnp.where(slot_index < listed, energy, jnp.zeros_like(energy))

        return lax.map(one_item, (jnp.arange(MAXP, dtype=jnp.int32), entries))

    pair_energy = lax.map(one_orbital, (jnp.arange(NOCC, dtype=jnp.int32), pair_list, pair_count))
    return pair_energy, jnp.sum(pair_energy)
```

```python
import jax
import jax.numpy as jnp
from jax import lax
from jax.experimental import pallas as pl
from jax.experimental.pallas import tpu as pltpu
from jax.sharding import Mesh
from jax.sharding import PartitionSpec as P

VB = 128
NV = 256
NOCC = 32
SLOTS = 16
LOW = SLOTS - 1
HALF = 128
OCC = ("occ_0", "occ_1", "occ_2")
AUX = ("aux_0", "aux_1")
NAMES = ("occ_0", "occ_1", "occ_2", "aux_0", "aux_1")
MESH = pl.DeviceIdType.MESH

UNITS = (
    ((0, 0), (0, 1), (0, 2)),
    ((0, 0), (0, 1), (1, 0), (1, 1), (1, 3), (0, 2), (1, 2)),
    ((0, 0), (0, 1), (1, 0), (1, 1), (1, 3), (2, 0), (2, 1), (2, 3),
     (0, 2), (1, 2), (2, 2), (3, 0), (3, 1), (3, 3), (3, 2)),
    ((0, 0), (0, 1), (1, 0), (1, 1), (1, 3), (0, 2), (1, 2), (3, 0), (3, 1), (3, 3), (3, 2)),
)
COUNT = (3, 7, 15, 11)
SECOND = (2, 5, 8, 5)
THIRD = (3, 7, 11, 7)
ROW_AT = ((0, 1, 3, 3), (-1, 0, 1, 1), (-1, -1, 0, -1), (-1, -1, 2, 0))


def packed(values):
    total = 0
    for place, value in enumerate(values):
        total += value * 4**place
    return total


U_TABLE = tuple(packed([u for u, _ in row]) for row in UNITS)
DX_TABLE = tuple(packed([dx for _, dx in row]) for row in UNITS)


def kernel(b_hbm, info_out, codes, vir, out, panels, info_in, parts, relay_out, relay_in, fin_out, fin_in,
           keep, hx_out, hx_in, vsum, acc, first_in, all_out, all_in,
           load_sem, x_send, x_recv, d_send, d_recv, z_send, z_recv, relay_send, relay_recv,
           fin_send, fin_recv, hx_send, hx_recv, tail_send, tail_recv):
    x, z, c, y, h = (lax.axis_index(name) for name in NAMES)
    me = (x * 4 + z) * 2 + c
    xs, zs, ys = ([(v + k) % 4 for k in range(4)] for v in (x, z, y))
    cs, hs = (c, 1 - c), (h, 1 - h)
    at_least_one = (z + 3) // 4
    at_least_two = z // 2
    at_three = z // 3

    def by_z(table):
        steps = [table[k + 1] - table[k] for k in range(3)]
        return table[0] + steps[0] * at_least_one + steps[1] * at_least_two + steps[2] * at_three

    x_next, x_prev, y_next, y_prev = xs[1], xs[3], ys[1], ys[3]
    dev_x = ((x_next, z, c, y, h), (x_prev, z, c, y, h))
    dev_y = ((x, z, c, y_next, h), (x, z, c, y_prev, h))
    dev_core = (x, z, 1 - c, y, h)
    dev_h = (x, z, c, y, 1 - h)

    others = []
    for k in range(1, NOCC):
        kx, kz, kc = k // 8, k // 2 % 4, k % 2
        there = (-kx % 4 * 4 + -kz % 4) * 2 + kc
        others.append((k, there, (xs[kx], zs[kz], cs[kc], y, h), (xs[kx] * 4 + zs[kz]) * 2 + cs[kc]))
    aux_others = []
    for k in range(1, 8):
        ky, kh = k // 2, k % 2
        aux_others.append((k, -ky % 4 * 2 + kh, (x, z, c, ys[ky], hs[kh])))

    def send(src, dst, send_sem, recv_sem, device):
        return pltpu.make_async_remote_copy(
            src_ref=src, dst_ref=dst, send_sem=send_sem, recv_sem=recv_sem,
            device_id=device, device_id_type=MESH)

    def wait_in(dst, recv_sem):
        send(dst, dst, x_send.at[0], recv_sem, dev_core).wait_recv()

    def wait_out(src, send_sem):
        send(src, src, send_sem, x_recv.at[0], dev_core).wait_send()

    def half(slot, part):
        return panels.at[slot, pl.ds(part * HALF, HALF)]

    load = pltpu.make_async_copy(b_hbm.at[0], panels.at[0], load_sem)
    load.start()

    barrier = pltpu.get_barrier_semaphore()

    for _, _, device, _ in others:
        pl.semaphore_signal(barrier, inc=1, device_id=device, device_id_type=MESH)
    for _, _, device in aux_others:
        pl.semaphore_signal(barrier, inc=1, device_id=device, device_id_type=MESH)
    load.wait()
    pl.semaphore_wait(barrier, NOCC - 1 + 7)

    own_x = (
        send(half(0, 0), half(3, 0), x_send.at[0], x_recv.at[0], dev_x[0]),
        send(half(0, 1), half(3, 1), x_send.at[1], x_recv.at[1], dev_x[0]),
        send(half(0, 1), half(1, 1), x_send.at[2], x_recv.at[2], dev_x[1]),
        send(half(0, 0), half(1, 0), x_send.at[3], x_recv.at[3], dev_x[1]),
    )
    passed_x = (
        send(half(3, 0), half(2, 0), x_send.at[4], x_recv.at[4], dev_x[0]),
        send(half(1, 1), half(2, 1), x_send.at[5], x_recv.at[5], dev_x[1]),
    )

    def core_copy(dx):
        return send(panels.at[dx], panels.at[4 + dx], d_send.at[dx], d_recv.at[dx], dev_core)

    def z_copy(slot, to_slot, part, to_z, kind):
        return send(half(slot, part), half(to_slot, part), z_send.at[kind, part],
                    z_recv.at[to_slot - 7, part], (x, to_z, c, y, h))

    own_z = {0: (0, 8, 1), 1: (0, 8, 2), 3: (0, 9, 2)}
    own_x[0].start()
    own_x[2].start()
    for from_z, (slot, to_slot, to_z) in own_z.items():
        @pl.when(z == from_z)
        def _(slot=slot, to_slot=to_slot, to_z=to_z):
            z_copy(slot, to_slot, 0, to_z, 0).start()
            z_copy(slot, to_slot, 1, to_z, 0).start()
    core_copy(0).start()
    own_x[1].start()
    own_x[3].start()

    for _, there, device, index in others:
        send(info_out.at[index], info_in.at[there], tail_send.at[0], tail_recv.at[0], device).start()
    info_in[0] = info_out[me]
    acc[...] = jnp.zeros_like(acc)

    wait_in(panels.at[4], d_recv.at[0])

    row_of = lax.broadcasted_iota(jnp.int32, (VB, VB), 0)
    lane_of = lax.broadcasted_iota(jnp.int32, (VB, VB), 1)
    left = vir[0:1, :]
    right = vir[1:2, :]

    def as_column(row_values, shift):
        wide = jnp.broadcast_to(row_values, (VB, VB))
        return jnp.sum(jnp.where(lane_of == shift, wide, 0.0), axis=1, keepdims=True)

    @pl.when(y == 0)
    def _():
        vsum[...] = as_column(left, row_of) + left

    @pl.when(y == 1)
    def _():
        vsum[...] = as_column(right, row_of) + right

    @pl.when(y == 2)
    def _():
        vsum[...] = as_column(left, row_of % 64) + right

    @pl.when(y == 3)
    def _():
        vsum[...] = as_column(left, row_of % 64 + 64) + right

    count = by_z(COUNT)
    second = by_z(SECOND)
    third = by_z(THIRD)

    def low_part(value):
        return (value - value.astype(jnp.bfloat16).astype(jnp.float32)).astype(jnp.bfloat16)

    def products(n, u, dx):
        row_slot = (7 + u) * ((u + 3) // 4)
        rows = panels[row_slot]
        for dc in range(2):
            block = lax.dot_general(rows, panels[dc * 4 + dx], (((1,), (1,)), ((), ())),
                                    preferred_element_type=jnp.float32)
            upper = block[:VB, VB:]
            lower = block[VB:, :VB].T
            parts[n, dc, 0] = block[:VB, :VB]
            parts[n, dc, 1] = block[VB:, VB:]
            parts[n, dc, 2, 0:64] = upper[:64]
            parts[n, dc, 2, 64:128] = lower[:64]
            parts[n, dc, 3, 0:64] = upper[64:]
            parts[n, dc, 3, 64:128] = lower[64:]
        far = ys[2]
        for dc in range(2):
            relay_out[n, dc] = parts[n, dc, far].astype(jnp.bfloat16)
            send(relay_out.at[n, dc], relay_in.at[n, dc], relay_send.at[n, dc], relay_recv.at[n, dc],
                 dev_y[dc]).start()

        @pl.when(n == 0)
        def _():
            relay_out[LOW, 0] = low_part(parts[0, 0, far])
            send(relay_out.at[LOW, 0], relay_in.at[LOW, 0], relay_send.at[LOW, 0], relay_recv.at[LOW, 0],
                 dev_y[0]).start()

    def pass_on_low():
        wait_in(relay_in.at[LOW, 0], relay_recv.at[LOW, 0])
        parts[0, 0, y_next] += relay_in[LOW, 0].astype(jnp.float32)
        fin_out[LOW, 0, 0] = low_part(parts[0, 0, y_next] + relay_in[0, 0].astype(jnp.float32))
        fin_out[LOW, 1, 0] = low_part(parts[0, 0, y_prev])
        for way in range(2):
            send(fin_out.at[LOW, way, 0], fin_in.at[LOW, way, 0], fin_send.at[LOW, way], fin_recv.at[LOW, way],
                 dev_y[way]).start()

    def pass_on(n):
        for dc in range(2):
            wait_in(relay_in.at[n, dc], relay_recv.at[n, dc])

        @pl.when(n == 0)
        def _():
            pass_on_low()

        fin_out[n, 0, 0] = (parts[n, 0, y_next] + relay_in[n, 0].astype(jnp.float32)).astype(jnp.bfloat16)
        fin_out[n, 0, 1] = parts[n, 1, y_next].astype(jnp.bfloat16)
        fin_out[n, 1, 0] = parts[n, 0, y_prev].astype(jnp.bfloat16)
        fin_out[n, 1, 1] = (parts[n, 1, y_prev] + relay_in[n, 1].astype(jnp.float32)).astype(jnp.bfloat16)
        for way in range(2):
            send(fin_out.at[n, way], fin_in.at[n, way], fin_send.at[n, way], fin_recv.at[n, way],
                 dev_y[way]).start()

    def cross(n):
        def summed(dc):
            return parts[n, dc, y] + fin_in[n, 0, dc].astype(jnp.float32) + fin_in[n, 1, dc].astype(jnp.float32)

        for way in range(2):
            wait_in(fin_in.at[n, way], fin_recv.at[n, way])

        @pl.when(n == 0)
        def _():
            for way in range(2):
                wait_in(fin_in.at[LOW, way, 0], fin_recv.at[LOW, way])
                parts[0, 0, y] += fin_in[LOW, way, 0].astype(jnp.float32)

            @pl.when(h == 1)
            def _():
                hx_out[LOW] = low_part(summed(0))
                send(hx_out.at[LOW], hx_in.at[LOW], hx_send.at[LOW], hx_recv.at[LOW], dev_h).start()

        hx_out[n] = summed(1 - h).astype(jnp.bfloat16)
        send(hx_out.at[n], hx_in.at[n], hx_send.at[n], hx_recv.at[n], dev_h).start()
        keep[n] = summed(h)

    lane_row = lax.broadcasted_iota(jnp.int32, (1, VB), 1)

    def energies(n, u, dx):
        wait_in(hx_in.at[n], hx_recv.at[n])

        @pl.when(n == 0)
        def _():
            @pl.when(h == 0)
            def _():
                wait_in(hx_in.at[LOW], hx_recv.at[LOW])
                keep[0] += hx_in[LOW].astype(jnp.float32)

        tile = keep[n] + hx_in[n].astype(jnp.float32)
        u_three = u // 3
        u_two = u // 2 - u_three
        u_one = (u + 3) // 4 - u // 2
        row_z = z * (1 - (u + 3) // 4) + u_one * at_least_two + u_two * 3
        row_energy = info_in[(row_z - z + 4) % 4 * 2][1:2, :]
        column_energy = info_in[dx * 8 + h][1:2, :]
        denominator = vsum[...] - row_energy - column_energy
        lane = u * 32 + (h * 4 + dx) * 4

        @pl.when(y < 2)
        def _():
            value = -jnp.sum(tile * (2.0 * tile - tile.T) / denominator, axis=0, keepdims=True)
            value = jnp.sum(value, axis=1, keepdims=True)
            acc[0:1, :] += jnp.where(lane_row == lane + 3 * y, value, 0.0)

        @pl.when(y >= 2)
        def _():
            top, bottom, under = tile[:64], tile[64:], denominator[:64]
            value = -jnp.sum(top * (2.0 * top - bottom) / under, axis=0, keepdims=True)
            other = -jnp.sum(bottom * (2.0 * bottom - top) / under, axis=0, keepdims=True)
            value = jnp.sum(value, axis=1, keepdims=True)
            other = jnp.sum(other, axis=1, keepdims=True)
            acc[0:1, :] += jnp.where(lane_row == lane + 1, value, 0.0) + jnp.where(lane_row == lane + 2, other, 0.0)

    def pass_rows(part, slot, to_slot, to_z, kind):
        wait_in(half(slot, part), z_recv.at[slot - 7, part])
        z_copy(slot, to_slot, part, to_z, kind).start()

    def first_arrivals():
        own_x[0].wait_recv()
        passed_x[0].start()
        own_x[2].wait_recv()
        passed_x[1].start()
        for part in range(2):
            @pl.when(z == 1)
            def _():
                pass_rows(part, 8, 10, 2, 1)

            @pl.when(z == 2)
            def _():
                pass_rows(part, 8, 8, 3, 1)

            if part == 0:
                own_x[1].wait_recv()
                core_copy(3).start()
                own_x[3].wait_recv()
                core_copy(1).start()
        wait_in(panels.at[7], d_recv.at[3])
        wait_in(panels.at[5], d_recv.at[1])

    def second_arrivals():
        passed_x[0].wait_recv()
        passed_x[1].wait_recv()
        core_copy(2).start()

        @pl.when(z == 2)
        def _():
            pass_rows(0, 10, 10, 3, 2)

        wait_in(panels.at[6], d_recv.at[2])

    def third_arrivals():
        @pl.when(z == 2)
        def _():
            pass_rows(1, 10, 10, 3, 2)

        @pl.when(z == 3)
        def _():
            for part in range(2):
                wait_in(half(10, part), z_recv.at[3, part])

    def each(low, high, action):
        def one(n, carry):
            action(n)
            return carry

        lax.fori_loop(low, high, one, 0)

    def step(n, carry):
        u_table, dx_table = carry
        products(n, u_table % 4, dx_table % 4)

        @pl.when(n == 0)
        def _():
            pass_on(0)
            first_arrivals()

        @pl.when(n == second - 1)
        def _():
            each(1, second, pass_on)
            second_arrivals()

        @pl.when(n == 1)
        def _():
            cross(0)

            @pl.when(z == 3)
            def _():
                for part in range(2):
                    wait_in(half(8, part), z_recv.at[1, part])

        @pl.when(n == 4)
        def _():
            @pl.when(z == 2)
            def _():
                for part in range(2):
                    wait_in(half(9, part), z_recv.at[2, part])

        @pl.when(n == third - 1)
        def _():
            @pl.when(z >= 2)
            def _():
                each(1, early, cross)
                third_arrivals()

        return (u_table // 4, dx_table // 4)

    start = jnp.int32(0)
    early = (second + 1) // 2
    crossed = 1 + (early - 1) * at_least_two
    lax.fori_loop(0, count, step, (start + by_z(U_TABLE), start + by_z(DX_TABLE)))
    each(second, count, pass_on)
    each(crossed, count, cross)
    wait_in(info_in.at[pl.ds(1, NOCC - 1)], tail_recv.at[0])

    def finish(n, carry):
        u_table, dx_table = carry
        energies(n, u_table % 4, dx_table % 4)
        return (u_table // 4, dx_table // 4)

    lax.fori_loop(0, count, finish, (start + by_z(U_TABLE), start + by_z(DX_TABLE)))

    for _, there, device in aux_others:
        send(acc, first_in.at[there], tail_send.at[1], tail_recv.at[1], device).start()
    weights = jnp.zeros((1, VB), jnp.float32)
    for k in range(NOCC):
        weights += info_in[k, 0:1, :]
    wait_in(first_in.at[pl.ds(1, 7)], tail_recv.at[1])
    mine = acc[0:1, :]
    for k in range(1, 8):
        mine += first_in[k, 0:1, :]
    all_out[0:1, :] = mine
    all_out[1:2, :] = mine * weights

    for _, there, device, _ in others:
        send(all_out, all_in.at[there], tail_send.at[2], tail_recv.at[2], device).start()
    wanted = codes[...]
    lanes = lax.broadcasted_iota(jnp.int32, (8, VB), 1)
    picked = jnp.where(wanted == me * VB + lanes, all_out[0:1, :], 0.0)
    total = all_out[1:2, :]

    for k in range(4):
        own_x[k].wait_send()
    for k in range(2):
        passed_x[k].wait_send()
    for dx in range(4):
        core_copy(dx).wait_send()
    for part in range(2):
        @pl.when(z != 2)
        def _():
            wait_out(half(0, part), z_send.at[0, part])

        @pl.when(z == 1)
        def _():
            wait_out(half(8, part), z_send.at[1, part])

        @pl.when(z == 2)
        def _():
            wait_out(half(8, part), z_send.at[1, part])
            wait_out(half(10, part), z_send.at[2, part])

    def sent(n, carry):
        for k in range(2):
            wait_out(relay_out.at[n, k], relay_send.at[n, k])
            wait_out(fin_out.at[n, k], fin_send.at[n, k])
        wait_out(hx_out.at[n], hx_send.at[n])
        return carry

    lax.fori_loop(0, count, sent, 0)
    wait_out(relay_out.at[LOW, 0], relay_send.at[LOW, 0])
    for way in range(2):
        wait_out(fin_out.at[LOW, way, 0], fin_send.at[LOW, way])

    @pl.when(h == 1)
    def _():
        wait_out(hx_out.at[LOW], hx_send.at[LOW])

    wait_out(info_in.at[pl.ds(1, NOCC - 1)], tail_send.at[0])
    wait_out(first_in.at[pl.ds(1, 7)], tail_send.at[1])

    wait_in(all_in.at[pl.ds(1, NOCC - 1)], tail_recv.at[2])
    for k, _, _, from_row in others:
        picked += jnp.where(wanted == from_row * VB + lanes, all_in[k, 0:1, :], 0.0)
        total += all_in[k, 1:2, :]
    sublane = lax.broadcasted_iota(jnp.int32, (8, VB), 0)
    picked = jnp.where(sublane == 6, jnp.broadcast_to(total, (8, VB)), picked)
    out[...] = jnp.broadcast_to(jnp.sum(picked, axis=1, keepdims=True), (8, VB))
    wait_out(all_in.at[pl.ds(1, NOCC - 1)], tail_send.at[2])


def place_codes(orbital, table, live):
    partner = jnp.maximum(table[:, 0], 0)
    left = jnp.maximum(table[:, 1], 0)
    right = jnp.maximum(table[:, 2], 0)

    def split(index):
        return index // 8, index // 2 % 4, index % 2

    xi, zi, ci = split(jnp.broadcast_to(orbital, partner.shape))
    xj, zj, cj = split(partner)

    def row_at(first, second):
        found = jnp.full(first.shape, -1, jnp.int32)
        for a in range(4):
            for b in range(4):
                if ROW_AT[a][b] >= 0:
                    found = jnp.where((first == a) & (second == b), ROW_AT[a][b], found)
        return found

    direct = row_at(zi, zj)
    ahead = (xj - xi) % 4
    swap = (direct < 0) | ((zi == zj) & (ahead == 3))
    unit = jnp.where(swap, row_at(zj, zi), direct)
    dx = jnp.where(swap, (4 - ahead) % 4, ahead)
    dc = (ci + cj) % 2
    quadrant = jnp.where(swap, right * 2 + left, left * 2 + right)
    row_x, row_c = jnp.where(swap, xj, xi), jnp.where(swap, cj, ci)
    column_z = jnp.where(swap, zi, zj)
    device = (row_x * 4 + column_z) * 2 + row_c
    lane = unit * 32 + (dc * 4 + dx) * 4 + quadrant
    return jnp.where(live, device * VB + lane, -1)


def local(b_factors, occ_energies, vir_energies, pair_list, pair_count):
    table = pair_list[0]
    slot_total = table.shape[0]
    orbital = lax.axis_index(OCC).astype(jnp.int32)
    share = slot_total // 8
    live = jnp.arange(slot_total, dtype=jnp.int32) < pair_count[0]
    codes = place_codes(orbital, table, live)
    device_hot = (codes[None, :] // VB == jnp.arange(NOCC, dtype=jnp.int32)[:, None]) & live[None, :]
    lane_hot = codes[:, None] % VB == jnp.arange(VB, dtype=jnp.int32)[None, :]
    weights = jnp.dot(device_hot.astype(jnp.bfloat16), lane_hot.astype(jnp.bfloat16),
                      preferred_element_type=jnp.float32)
    sub = lax.broadcasted_iota(jnp.int32, (NOCC, 8, VB), 1)
    info = jnp.where(sub == 0, weights[:, None, :], occ_energies[0])
    mine = lax.dynamic_slice_in_dim(codes, lax.axis_index(AUX) * share, share, 0)
    mine = jnp.concatenate([mine, jnp.full((8 - share,), -1, jnp.int32)])
    mine = jnp.broadcast_to(mine[:, None], (8, VB))
    vmem = pl.BlockSpec(memory_space=pltpu.VMEM)
    bf16, f32 = jnp.bfloat16, jnp.float32
    dma = pltpu.SemaphoreType.DMA
    tile = (VB, VB)
    result = pl.pallas_call(
        kernel,
        out_shape=jax.ShapeDtypeStruct((8, VB), f32),
        in_specs=[pl.BlockSpec(memory_space=pl.ANY), vmem, vmem, vmem],
        out_specs=vmem,
        scratch_shapes=[
            pltpu.VMEM((11, *b_factors.shape[1:]), bf16),
            pltpu.VMEM((NOCC, 8, VB), f32),
            pltpu.VMEM((SLOTS, 2, 4, *tile), f32),
            pltpu.VMEM((SLOTS, 2, *tile), bf16),
            pltpu.VMEM((SLOTS, 2, *tile), bf16),
            pltpu.VMEM((SLOTS, 2, 2, *tile), bf16),
            pltpu.VMEM((SLOTS, 2, 2, *tile), bf16),
            pltpu.VMEM((SLOTS, *tile), f32),
            pltpu.VMEM((SLOTS, *tile), bf16),
            pltpu.VMEM((SLOTS, *tile), bf16),
            pltpu.VMEM(tile, f32),
            pltpu.VMEM((8, VB), f32),
            pltpu.VMEM((8, 8, VB), f32),
            pltpu.VMEM((8, VB), f32),
            pltpu.VMEM((NOCC, 8, VB), f32),
            dma, dma((6,)), dma((6,)), dma((4,)), dma((4,)), dma((3, 2)), dma((4, 2)),
            dma((SLOTS, 2)), dma((SLOTS, 2)), dma((SLOTS, 2)), dma((SLOTS, 2)),
            dma((SLOTS,)), dma((SLOTS,)), dma((3,)), dma((3,)),
        ],
        compiler_params=pltpu.CompilerParams(collective_id=0, has_side_effects=True),
        name="pair_energies",
    )(b_factors, info, mine, vir_energies.reshape(2, VB))
    return result[:share, 0][None, :], result[6, 0]


def solution(mesh):
    finer = Mesh(mesh.devices.reshape(4, 4, 2, 4, 2), NAMES)
    placed = (P(OCC, None, AUX), P(OCC), P(), P(OCC, None, None), P(OCC))
    return jax.shard_map(
        local, mesh=finer, in_specs=placed, out_specs=(P(OCC, AUX), P()), check_vma=False
    )
```

```python
import jax
import jax.numpy as jnp
from jax import lax
from jax.experimental import pallas as pl
from jax.experimental.pallas import tpu as pltpu
from jax.sharding import Mesh
from jax.sharding import PartitionSpec as P

VB = 128
NV = 256
NOCC = 32
SLOTS = 12
LOW = SLOTS - 1
HALF = 128
OCC = ("occ_0", "occ_1", "occ_2")
AUX = ("aux_0", "aux_1")
NAMES = ("occ_0", "occ_1", "occ_2", "aux_0", "aux_1")
MESH = pl.DeviceIdType.MESH

UNITS = (
    ((0, 0), (0, 1), (0, 2), (2, 0), (2, 1), (2, 3), (2, 2)),
    ((0, 0), (0, 1), (1, 0), (1, 1), (1, 3), (0, 2), (1, 2), (2, 0), (2, 1), (2, 3), (2, 2)),
    ((0, 0), (0, 1), (1, 0), (1, 1), (1, 3), (0, 2), (1, 2), (2, 0), (2, 1), (2, 3), (2, 2)),
    ((0, 0), (0, 1), (1, 0), (1, 1), (1, 3), (0, 2), (1, 2)),
)
COUNT = (7, 11, 11, 7)
SECOND = (2, 5, 5, 5)
THIRD = (3, 7, 7, 7)
MOVES = ((0, 1, 1), (1, 2, 1), (2, 3, 1), (3, 1, 2), (0, 2, 2), (3, 0, 2))
ROW_AT = ((0, 1, 2, -1), (-1, 0, 1, -1), (-1, -1, 0, 1), (2, 2, -1, 0))


def packed(values):
    total = 0
    for place, value in enumerate(values):
        total += value * 4**place
    return total


U_TABLE = tuple(packed([u for u, _ in row]) for row in UNITS)
DX_TABLE = tuple(packed([dx for _, dx in row]) for row in UNITS)


def kernel(b_hbm, info_out, codes, vir, out, total_out, panels, info_in, parts, relay_out, relay_in, fin_out, fin_in,
           keep, hx_out, hx_in, vsum, acc, first_in, all_out, all_in,
           load_sem, x_send, x_recv, d_send, d_recv, z_send, z_recv, relay_send, relay_recv,
           fin_send, fin_recv, hx_send, hx_recv, tail_send, tail_recv):
    x, z, c, y, h = (lax.axis_index(name) for name in NAMES)
    me = (x * 4 + z) * 2 + c
    xs, zs, ys = ([(v + k) % 4 for k in range(4)] for v in (x, z, y))
    cs, hs = (c, 1 - c), (h, 1 - h)
    at_least_one = (z + 3) // 4
    at_least_two = z // 2
    at_three = z // 3

    def by_z(table):
        steps = [table[k + 1] - table[k] for k in range(3)]
        return table[0] + steps[0] * at_least_one + steps[1] * at_least_two + steps[2] * at_three

    x_next, x_prev, y_next, y_prev = xs[1], xs[3], ys[1], ys[3]
    dev_x = ((x_next, z, c, y, h), (x_prev, z, c, y, h))
    dev_y = ((x, z, c, y_next, h), (x, z, c, y_prev, h))
    dev_core = (x, z, 1 - c, y, h)
    dev_h = (x, z, c, y, 1 - h)

    others = []
    for k in range(1, NOCC):
        kx, kz, kc = k // 8, k // 2 % 4, k % 2
        there = (-kx % 4 * 4 + -kz % 4) * 2 + kc
        others.append((k, there, (xs[kx], zs[kz], cs[kc], y, h), (xs[kx] * 4 + zs[kz]) * 2 + cs[kc]))
    aux_others = []
    for k in range(1, 8):
        ky, kh = k // 2, k % 2
        aux_others.append((k, -ky % 4 * 2 + kh, (x, z, c, ys[ky], hs[kh])))

    def send(src, dst, send_sem, recv_sem, device):
        return pltpu.make_async_remote_copy(
            src_ref=src, dst_ref=dst, send_sem=send_sem, recv_sem=recv_sem,
            device_id=device, device_id_type=MESH)

    def wait_in(dst, recv_sem):
        send(dst, dst, x_send.at[0], recv_sem, dev_core).wait_recv()

    def wait_out(src, send_sem):
        send(src, src, send_sem, x_recv.at[0], dev_core).wait_send()

    def half(slot, part):
        return panels.at[slot, pl.ds(part * HALF, HALF)]

    load = pltpu.make_async_copy(b_hbm.at[0], panels.at[0], load_sem)
    load.start()

    barrier = pltpu.get_barrier_semaphore()

    for _, _, device, _ in others:
        pl.semaphore_signal(barrier, inc=1, device_id=device, device_id_type=MESH)
    for _, _, device in aux_others:
        pl.semaphore_signal(barrier, inc=1, device_id=device, device_id_type=MESH)
    load.wait()
    pl.semaphore_wait(barrier, NOCC - 1 + 7)

    own_x = (
        send(half(0, 0), half(3, 0), x_send.at[0], x_recv.at[0], dev_x[0]),
        send(half(0, 1), half(3, 1), x_send.at[1], x_recv.at[1], dev_x[0]),
        send(half(0, 1), half(1, 1), x_send.at[2], x_recv.at[2], dev_x[1]),
        send(half(0, 0), half(1, 0), x_send.at[3], x_recv.at[3], dev_x[1]),
    )
    passed_x = (
        send(half(3, 0), half(2, 0), x_send.at[4], x_recv.at[4], dev_x[0]),
        send(half(1, 1), half(2, 1), x_send.at[5], x_recv.at[5], dev_x[1]),
    )

    def core_copy(dx):
        return send(panels.at[dx], panels.at[4 + dx], d_send.at[dx], d_recv.at[dx], dev_core)

    def z_copy(to_z, u, kind):
        return send(panels.at[0], panels.at[7 + u], z_send.at[kind], z_recv.at[u], (x, to_z, c, y, h))

    own_x[0].start()
    own_x[2].start()
    for index, (from_z, to_z, u) in enumerate(MOVES):
        @pl.when(z == from_z)
        def _(to_z=to_z, u=u, kind=index // 4):
            z_copy(to_z, u, kind).start()

    core_copy(0).start()
    own_x[1].start()
    own_x[3].start()

    for _, there, device, index in others:
        send(info_out.at[index], info_in.at[there], tail_send.at[0], tail_recv.at[0], device).start()
    info_in[0] = info_out[me]
    acc[...] = jnp.zeros_like(acc)

    wait_in(panels.at[4], d_recv.at[0])

    row_of = lax.broadcasted_iota(jnp.int32, (VB, VB), 0)
    lane_of = lax.broadcasted_iota(jnp.int32, (VB, VB), 1)
    left = vir[0:1, :]
    right = vir[1:2, :]

    def as_column(row_values, shift):
        wide = jnp.broadcast_to(row_values, (VB, VB))
        return jnp.sum(jnp.where(lane_of == shift, wide, 0.0), axis=1, keepdims=True)

    @pl.when(y == 0)
    def _():
        vsum[...] = as_column(left, row_of) + left

    @pl.when(y == 1)
    def _():
        vsum[...] = as_column(right, row_of) + right

    @pl.when(y == 2)
    def _():
        vsum[...] = as_column(left, row_of % 64) + right

    @pl.when(y == 3)
    def _():
        vsum[...] = as_column(left, row_of % 64 + 64) + right

    count = by_z(COUNT)
    second = by_z(SECOND)
    third = by_z(THIRD)

    def low_part(value):
        return (value - value.astype(jnp.bfloat16).astype(jnp.float32)).astype(jnp.bfloat16)

    def products(n, u, dx):
        row_slot = (7 + u) * ((u + 3) // 4)
        rows = panels[row_slot]
        for dc in range(2):
            block = lax.dot_general(rows, panels[dc * 4 + dx], (((1,), (1,)), ((), ())),
                                    preferred_element_type=jnp.float32)
            upper = block[:VB, VB:]
            lower = block[VB:, :VB].T
            parts[n, dc, 0] = block[:VB, :VB]
            parts[n, dc, 1] = block[VB:, VB:]
            parts[n, dc, 2, 0:64] = upper[:64]
            parts[n, dc, 2, 64:128] = lower[:64]
            parts[n, dc, 3, 0:64] = upper[64:]
            parts[n, dc, 3, 64:128] = lower[64:]
        far = ys[2]
        for dc in range(2):
            relay_out[n, dc] = parts[n, dc, far].astype(jnp.bfloat16)
            send(relay_out.at[n, dc], relay_in.at[n, dc], relay_send.at[n, dc], relay_recv.at[n, dc],
                 dev_y[dc]).start()

        @pl.when(n == 0)
        def _():
            relay_out[LOW, 0] = low_part(parts[0, 0, far])
            send(relay_out.at[LOW, 0], relay_in.at[LOW, 0], relay_send.at[LOW, 0], relay_recv.at[LOW, 0],
                 dev_y[0]).start()

    def pass_on_low():
        wait_in(relay_in.at[LOW, 0], relay_recv.at[LOW, 0])
        parts[0, 0, y_next] += relay_in[LOW, 0].astype(jnp.float32)
        fin_out[LOW, 0, 0] = low_part(parts[0, 0, y_next] + relay_in[0, 0].astype(jnp.float32))
        fin_out[LOW, 1, 0] = low_part(parts[0, 0, y_prev])
        for way in range(2):
            send(fin_out.at[LOW, way, 0], fin_in.at[LOW, way, 0], fin_send.at[LOW, way], fin_recv.at[LOW, way],
                 dev_y[way]).start()

    def pass_on(n):
        for dc in range(2):
            wait_in(relay_in.at[n, dc], relay_recv.at[n, dc])

        @pl.when(n == 0)
        def _():
            pass_on_low()

        fin_out[n, 0, 0] = (parts[n, 0, y_next] + relay_in[n, 0].astype(jnp.float32)).astype(jnp.bfloat16)
        fin_out[n, 0, 1] = parts[n, 1, y_next].astype(jnp.bfloat16)
        fin_out[n, 1, 0] = parts[n, 0, y_prev].astype(jnp.bfloat16)
        fin_out[n, 1, 1] = (parts[n, 1, y_prev] + relay_in[n, 1].astype(jnp.float32)).astype(jnp.bfloat16)
        for way in range(2):
            send(fin_out.at[n, way], fin_in.at[n, way], fin_send.at[n, way], fin_recv.at[n, way],
                 dev_y[way]).start()

    def cross(n):
        def summed(dc):
            return parts[n, dc, y] + fin_in[n, 0, dc].astype(jnp.float32) + fin_in[n, 1, dc].astype(jnp.float32)

        for way in range(2):
            wait_in(fin_in.at[n, way], fin_recv.at[n, way])

        @pl.when(n == 0)
        def _():
            for way in range(2):
                wait_in(fin_in.at[LOW, way, 0], fin_recv.at[LOW, way])
                parts[0, 0, y] += fin_in[LOW, way, 0].astype(jnp.float32)

            @pl.when(h == 1)
            def _():
                hx_out[LOW] = low_part(summed(0))
                send(hx_out.at[LOW], hx_in.at[LOW], hx_send.at[LOW], hx_recv.at[LOW], dev_h).start()

        hx_out[n] = summed(1 - h).astype(jnp.bfloat16)
        send(hx_out.at[n], hx_in.at[n], hx_send.at[n], hx_recv.at[n], dev_h).start()
        keep[n] = summed(h)

    lane_row = lax.broadcasted_iota(jnp.int32, (1, VB), 1)

    def energies(n, u, dx):
        wait_in(hx_in.at[n], hx_recv.at[n])

        @pl.when(n == 0)
        def _():
            @pl.when(h == 0)
            def _():
                wait_in(hx_in.at[LOW], hx_recv.at[LOW])
                keep[0] += hx_in[LOW].astype(jnp.float32)

        tile = keep[n] + hx_in[n].astype(jnp.float32)
        first = u % 2 * (z - 1)
        second_row = u // 2 * (3 - 3 * (at_least_two - at_three))
        row_z = z * (1 - (u + 1) // 2) + first + second_row
        row_energy = info_in[(row_z - z + 4) % 4 * 2][1:2, :]
        column_energy = info_in[dx * 8 + h][1:2, :]
        denominator = vsum[...] - row_energy - column_energy
        lane = u * 32 + (h * 4 + dx) * 4

        @pl.when(y < 2)
        def _():
            value = -jnp.sum(tile * (2.0 * tile - tile.T) / denominator, axis=0, keepdims=True)
            value = jnp.sum(value, axis=1, keepdims=True)
            acc[0:1, :] += jnp.where(lane_row == lane + 3 * y, value, 0.0)

        @pl.when(y >= 2)
        def _():
            top, bottom, under = tile[:64], tile[64:], denominator[:64]
            value = -jnp.sum(top * (2.0 * top - bottom) / under, axis=0, keepdims=True)
            other = -jnp.sum(bottom * (2.0 * bottom - top) / under, axis=0, keepdims=True)
            value = jnp.sum(value, axis=1, keepdims=True)
            other = jnp.sum(other, axis=1, keepdims=True)
            acc[0:1, :] += jnp.where(lane_row == lane + 1, value, 0.0) + jnp.where(lane_row == lane + 2, other, 0.0)

    def first_arrivals():
        own_x[0].wait_recv()
        passed_x[0].start()
        own_x[2].wait_recv()
        passed_x[1].start()

    def second_arrivals():
        own_x[1].wait_recv()
        core_copy(3).start()
        own_x[3].wait_recv()
        core_copy(1).start()
        wait_in(panels.at[7], d_recv.at[3])
        wait_in(panels.at[5], d_recv.at[1])

        @pl.when(z >= 1)
        def _():
            wait_in(panels.at[8], z_recv.at[1])

    def third_arrivals():
        passed_x[0].wait_recv()
        passed_x[1].wait_recv()
        core_copy(2).start()
        wait_in(panels.at[6], d_recv.at[2])

    def each(low, high, action):
        def one(n, carry):
            action(n)
            return carry

        lax.fori_loop(low, high, one, 0)

    def step(n, carry):
        u_table, dx_table = carry
        products(n, u_table % 4, dx_table % 4)

        @pl.when(n == 0)
        def _():
            pass_on(0)
            first_arrivals()
            cross(0)
            second_arrivals()

        @pl.when(n == second - 1)
        def _():
            each(1, second, pass_on)
            third_arrivals()

        @pl.when(n == third - 1)
        def _():
            each(second, third, pass_on)
            each(1, second, cross)

            @pl.when(z <= 2)
            def _():
                wait_in(panels.at[9], z_recv.at[2])

        return (u_table // 4, dx_table // 4)

    start = jnp.int32(0)
    lax.fori_loop(0, count, step, (start + by_z(U_TABLE), start + by_z(DX_TABLE)))
    each(third, count, pass_on)
    each(second, third, cross)
    wait_in(info_in.at[pl.ds(1, NOCC - 1)], tail_recv.at[0])

    def finish(n, carry):
        u_table, dx_table = carry
        energies(n, u_table % 4, dx_table % 4)
        return (u_table // 4, dx_table // 4)

    tables = lax.fori_loop(0, second, finish, (start + by_z(U_TABLE), start + by_z(DX_TABLE)))
    each(third, count, cross)
    lax.fori_loop(second, count, finish, tables)

    for _, there, device in aux_others:
        send(acc, first_in.at[there], tail_send.at[1], tail_recv.at[1], device).start()
    weights = jnp.zeros((1, VB), jnp.float32)
    for k in range(NOCC):
        weights += info_in[k, 0:1, :]
    wait_in(first_in.at[pl.ds(1, 7)], tail_recv.at[1])
    mine = acc[0:1, :]
    for k in range(1, 8):
        mine += first_in[k, 0:1, :]
    all_out[0:1, :] = mine
    all_out[1:2, :] = mine * weights

    for _, there, device, _ in others:
        send(all_out, all_in.at[there], tail_send.at[2], tail_recv.at[2], device).start()
    wanted = codes[...]
    lanes = lax.broadcasted_iota(jnp.int32, (8, VB), 1)
    picked = jnp.where(wanted == me * VB + lanes, all_out[0:1, :], 0.0)
    total = all_out[1:2, :]

    for k in range(4):
        own_x[k].wait_send()
    for k in range(2):
        passed_x[k].wait_send()
    for dx in range(4):
        core_copy(dx).wait_send()
    wait_out(panels.at[0], z_send.at[0])

    @pl.when(z % 3 == 0)
    def _():
        wait_out(panels.at[0], z_send.at[1])

    def sent(n, carry):
        for k in range(2):
            wait_out(relay_out.at[n, k], relay_send.at[n, k])
            wait_out(fin_out.at[n, k], fin_send.at[n, k])
        wait_out(hx_out.at[n], hx_send.at[n])
        return carry

    lax.fori_loop(0, count, sent, 0)
    wait_out(relay_out.at[LOW, 0], relay_send.at[LOW, 0])
    for way in range(2):
        wait_out(fin_out.at[LOW, way, 0], fin_send.at[LOW, way])

    @pl.when(h == 1)
    def _():
        wait_out(hx_out.at[LOW], hx_send.at[LOW])

    wait_out(info_in.at[pl.ds(1, NOCC - 1)], tail_send.at[0])
    wait_out(first_in.at[pl.ds(1, 7)], tail_send.at[1])

    wait_in(all_in.at[pl.ds(1, NOCC - 1)], tail_recv.at[2])
    for k, _, _, from_row in others:
        picked += jnp.where(wanted == from_row * VB + lanes, all_in[k, 0:1, :], 0.0)
        total += all_in[k, 1:2, :]
    sublane = lax.broadcasted_iota(jnp.int32, (8, VB), 0)
    picked = jnp.sum(picked, axis=1, keepdims=True)
    picked = jnp.sum(jnp.where(sublane == lanes, picked, 0.0), axis=0, keepdims=True)
    out[...] = picked[:, : out.shape[1]]
    total_out[...] = jnp.sum(total, axis=1, keepdims=True)
    wait_out(all_in.at[pl.ds(1, NOCC - 1)], tail_send.at[2])


def place_codes(orbital, table, live):
    partner = jnp.maximum(table[:, 0], 0)
    left = jnp.maximum(table[:, 1], 0)
    right = jnp.maximum(table[:, 2], 0)

    def split(index):
        return index // 8, index // 2 % 4, index % 2

    xi, zi, ci = split(jnp.broadcast_to(orbital, partner.shape))
    xj, zj, cj = split(partner)

    def row_at(first, second):
        found = jnp.full(first.shape, -1, jnp.int32)
        for a in range(4):
            for b in range(4):
                if ROW_AT[a][b] >= 0:
                    found = jnp.where((first == a) & (second == b), ROW_AT[a][b], found)
        return found

    direct = row_at(zi, zj)
    ahead = (xj - xi) % 4
    swap = (direct < 0) | ((zi == zj) & (ahead == 3))
    unit = jnp.where(swap, row_at(zj, zi), direct)
    dx = jnp.where(swap, (4 - ahead) % 4, ahead)
    dc = (ci + cj) % 2
    quadrant = jnp.where(swap, right * 2 + left, left * 2 + right)
    row_x, row_c = jnp.where(swap, xj, xi), jnp.where(swap, cj, ci)
    column_z = jnp.where(swap, zi, zj)
    device = (row_x * 4 + column_z) * 2 + row_c
    lane = unit * 32 + (dc * 4 + dx) * 4 + quadrant
    return jnp.where(live, device * VB + lane, -1)


def local(b_factors, occ_energies, vir_energies, pair_list, pair_count):
    table = pair_list[0]
    slot_total = table.shape[0]
    orbital = lax.axis_index(OCC).astype(jnp.int32)
    share = slot_total // 8
    live = jnp.arange(slot_total, dtype=jnp.int32) < pair_count[0]
    codes = place_codes(orbital, table, live)
    device_hot = (codes[None, :] // VB == jnp.arange(NOCC, dtype=jnp.int32)[:, None]) & live[None, :]
    lane_hot = codes[:, None] % VB == jnp.arange(VB, dtype=jnp.int32)[None, :]
    weights = jnp.dot(device_hot.astype(jnp.bfloat16), lane_hot.astype(jnp.bfloat16),
                      preferred_element_type=jnp.float32)
    sub = lax.broadcasted_iota(jnp.int32, (NOCC, 8, VB), 1)
    info = jnp.where(sub == 0, weights[:, None, :], occ_energies[0])
    mine = lax.dynamic_slice_in_dim(codes, lax.axis_index(AUX) * share, share, 0)
    mine = jnp.concatenate([mine, jnp.full((8 - share,), -1, jnp.int32)])
    mine = jnp.broadcast_to(mine[:, None], (8, VB))
    vmem = pl.BlockSpec(memory_space=pltpu.VMEM)
    bf16, f32 = jnp.bfloat16, jnp.float32
    dma = pltpu.SemaphoreType.DMA
    tile = (VB, VB)
    pair_energy, total_energy = pl.pallas_call(
        kernel,
        out_shape=(jax.ShapeDtypeStruct((1, share), f32), jax.ShapeDtypeStruct((1, 1), f32)),
        in_specs=[pl.BlockSpec(memory_space=pl.ANY), vmem, vmem, vmem],
        out_specs=(vmem, vmem),
        scratch_shapes=[
            pltpu.VMEM((10, *b_factors.shape[1:]), bf16),
            pltpu.VMEM((NOCC, 8, VB), f32),
            pltpu.VMEM((SLOTS, 2, 4, *tile), f32),
            pltpu.VMEM((SLOTS, 2, *tile), bf16),
            pltpu.VMEM((SLOTS, 2, *tile), bf16),
            pltpu.VMEM((SLOTS, 2, 2, *tile), bf16),
            pltpu.VMEM((SLOTS, 2, 2, *tile), bf16),
            pltpu.VMEM((SLOTS, *tile), f32),
            pltpu.VMEM((SLOTS, *tile), bf16),
            pltpu.VMEM((SLOTS, *tile), bf16),
            pltpu.VMEM(tile, f32),
            pltpu.VMEM((8, VB), f32),
            pltpu.VMEM((8, 8, VB), f32),
            pltpu.VMEM((8, VB), f32),
            pltpu.VMEM((NOCC, 8, VB), f32),
            dma, dma((6,)), dma((6,)), dma((4,)), dma((4,)), dma((2,)), dma((3,)),
            dma((SLOTS, 2)), dma((SLOTS, 2)), dma((SLOTS, 2)), dma((SLOTS, 2)),
            dma((SLOTS,)), dma((SLOTS,)), dma((3,)), dma((3,)),
        ],
        compiler_params=pltpu.CompilerParams(collective_id=0, has_side_effects=True),
        name="pair_energies",
    )(b_factors, info, mine, vir_energies.reshape(2, VB))
    return pair_energy, total_energy[0, 0]


def solution(mesh):
    finer = Mesh(mesh.devices.reshape(4, 4, 2, 4, 2), NAMES)
    placed = (P(OCC, None, AUX), P(OCC), P(), P(OCC, None, None), P(OCC))
    return jax.shard_map(
        local, mesh=finer, in_specs=placed, out_specs=(P(OCC, AUX), P()), check_vma=False
    )
```

```python
import jax
import jax.numpy as jnp
from jax import lax
from jax.experimental import pallas as pl
from jax.experimental.pallas import tpu as pltpu
from jax.sharding import Mesh
from jax.sharding import PartitionSpec as P

VB = 128
NV = 256
NOCC = 32
SLOTS = 12
LOW = SLOTS - 1
HALF = 128
OCC = ("occ_0", "occ_1", "occ_2")
AUX = ("aux_0", "aux_1")
NAMES = ("occ_0", "occ_1", "occ_2", "aux_0", "aux_1")
MESH = pl.DeviceIdType.MESH

UNITS = (
    ((0, 0), (0, 1), (0, 2), (2, 0), (2, 1), (2, 3), (2, 2)),
    ((0, 0), (0, 1), (1, 0), (1, 1), (1, 3), (0, 2), (1, 2), (2, 0), (2, 1), (2, 3), (2, 2)),
    ((0, 0), (0, 1), (1, 0), (1, 1), (1, 3), (0, 2), (1, 2), (2, 0), (2, 1), (2, 3), (2, 2)),
    ((0, 0), (0, 1), (1, 0), (1, 1), (1, 3), (0, 2), (1, 2)),
)
COUNT = (7, 11, 11, 7)
SECOND = (2, 5, 5, 5)
THIRD = (3, 7, 7, 7)
MOVES = ((0, 1, 1), (1, 2, 1), (2, 3, 1), (3, 1, 2), (0, 2, 2), (3, 0, 2))
ROW_AT = ((0, 1, 2, -1), (-1, 0, 1, -1), (-1, -1, 0, 1), (2, 2, -1, 0))


def packed(values):
    total = 0
    for place, value in enumerate(values):
        total += value * 4**place
    return total


U_TABLE = tuple(packed([u for u, _ in row]) for row in UNITS)
DX_TABLE = tuple(packed([dx for _, dx in row]) for row in UNITS)


def kernel(b_hbm, info_out, codes, vir, out, total_out, panels, info_in, parts, relay_out, relay_in, fin_out, fin_in,
           keep, hx_out, hx_in, vsum, acc, first_in, all_out, all_in,
           load_sem, x_send, x_recv, d_send, d_recv, z_send, z_recv, relay_send, relay_recv,
           fin_send, fin_recv, hx_send, hx_recv, tail_send, tail_recv, turn):
    x, z, c, y, h = (lax.axis_index(name) for name in NAMES)
    me = (x * 4 + z) * 2 + c
    xs, zs, ys = ([(v + k) % 4 for k in range(4)] for v in (x, z, y))
    cs, hs = (c, 1 - c), (h, 1 - h)
    at_least_one = (z + 3) // 4
    at_least_two = z // 2
    at_three = z // 3

    def by_z(table):
        steps = [table[k + 1] - table[k] for k in range(3)]
        return table[0] + steps[0] * at_least_one + steps[1] * at_least_two + steps[2] * at_three

    x_next, x_prev, y_next, y_prev = xs[1], xs[3], ys[1], ys[3]
    dev_x = ((x_next, z, c, y, h), (x_prev, z, c, y, h))
    dev_y = ((x, z, c, y_next, h), (x, z, c, y_prev, h))
    dev_core = (x, z, 1 - c, y, h)
    dev_h = (x, z, c, y, 1 - h)

    others = []
    for k in range(1, NOCC):
        kx, kz, kc = k // 8, k // 2 % 4, k % 2
        there = (-kx % 4 * 4 + -kz % 4) * 2 + kc
        others.append((k, there, (xs[kx], zs[kz], cs[kc], y, h), (xs[kx] * 4 + zs[kz]) * 2 + cs[kc]))
    plane = [(k, -(k // 4) % 4 * 4 + -k % 4, (xs[k // 4], z, c, ys[k % 4], h)) for k in range(1, 16)]
    column = [(k, (-(k // 4) % 4 * 2 + k // 2 % 2) * 2 + k % 2, (x, zs[k // 4], cs[k % 2], y, hs[k // 2 % 2]))
              for k in range(1, 16)]
    greeted = [device for _, _, device, _ in others] + [dev_h]
    greeted += [device for k, _, device in plane if k % 4 != 0]
    greeted += [device for k, _, device in column if k // 2 % 2 == 1 and k != 2]

    def send(src, dst, send_sem, recv_sem, device):
        return pltpu.make_async_remote_copy(
            src_ref=src, dst_ref=dst, send_sem=send_sem, recv_sem=recv_sem,
            device_id=device, device_id_type=MESH)

    def wait_in(dst, recv_sem):
        send(dst, dst, x_send.at[0], recv_sem, dev_core).wait_recv()

    def wait_out(src, send_sem):
        send(src, src, send_sem, x_recv.at[0], dev_core).wait_send()

    def half(slot, part):
        return panels.at[slot, pl.ds(part * HALF, HALF)]

    load = pltpu.make_async_copy(b_hbm.at[0], panels.at[0], load_sem)
    load.start()

    barrier = pltpu.get_barrier_semaphore()

    for device in greeted:
        pl.semaphore_signal(barrier, inc=1, device_id=device, device_id_type=MESH)
    load.wait()
    pl.semaphore_wait(barrier, len(greeted))

    own_x = (
        send(half(0, 0), half(3, 0), x_send.at[0], x_recv.at[0], dev_x[0]),
        send(half(0, 1), half(3, 1), x_send.at[1], x_recv.at[1], dev_x[0]),
        send(half(0, 1), half(1, 1), x_send.at[2], x_recv.at[2], dev_x[1]),
        send(half(0, 0), half(1, 0), x_send.at[3], x_recv.at[3], dev_x[1]),
    )
    passed_x = (
        send(half(3, 0), half(2, 0), x_send.at[4], x_recv.at[4], dev_x[0]),
        send(half(1, 1), half(2, 1), x_send.at[5], x_recv.at[5], dev_x[1]),
    )

    def core_copy(dx):
        return send(panels.at[dx], panels.at[4 + dx], d_send.at[dx], d_recv.at[dx], dev_core)

    def z_copy(to_z, u, kind):
        return send(panels.at[0], panels.at[7 + u], z_send.at[kind], z_recv.at[u], (x, to_z, c, y, h))

    own_x[0].start()
    own_x[2].start()
    for index, (from_z, to_z, u) in enumerate(MOVES):
        @pl.when(z == from_z)
        def _(to_z=to_z, u=u, kind=index // 4):
            if kind == 0:
                z_copy(to_z, u, kind).start()
            else:
                @pl.when(c == 0)
                def _():
                    z_copy(to_z, u, kind).start()

    core_copy(0).start()
    own_x[1].start()
    own_x[3].start()

    for _, there, device, index in others:
        send(info_out.at[index], info_in.at[there], tail_send.at[0], tail_recv.at[0], device).start()
    info_in[0] = info_out[me]
    acc[...] = jnp.zeros_like(acc)

    wait_in(panels.at[4], d_recv.at[0])

    row_of = lax.broadcasted_iota(jnp.int32, (VB, VB), 0)
    lane_of = lax.broadcasted_iota(jnp.int32, (VB, VB), 1)
    left = vir[0:1, :]
    right = vir[1:2, :]

    def as_column(row_values, shift):
        wide = jnp.broadcast_to(row_values, (VB, VB))
        return jnp.sum(jnp.where(lane_of == shift, wide, 0.0), axis=1, keepdims=True)

    @pl.when(y == 0)
    def _():
        vsum[...] = as_column(left, row_of) + left

    @pl.when(y == 1)
    def _():
        vsum[...] = as_column(right, row_of) + right

    @pl.when(y == 2)
    def _():
        vsum[...] = as_column(left, row_of % 64) + right

    @pl.when(y == 3)
    def _():
        vsum[...] = as_column(left, row_of % 64 + 64) + right

    count = by_z(COUNT)
    second = by_z(SECOND)
    third = by_z(THIRD)

    def low_part(value):
        return (value - value.astype(jnp.bfloat16).astype(jnp.float32)).astype(jnp.bfloat16)

    def products(n, u, dx):
        row_slot = (7 + u) * ((u + 3) // 4)
        rows = panels[row_slot]
        for dc in range(2):
            block = lax.dot_general(rows, panels[dc * 4 + dx], (((1,), (1,)), ((), ())),
                                    preferred_element_type=jnp.float32)
            upper = block[:VB, VB:]
            lower = block[VB:, :VB].T
            parts[n, dc, 0] = block[:VB, :VB]
            parts[n, dc, 1] = block[VB:, VB:]
            parts[n, dc, 2, 0:64] = upper[:64]
            parts[n, dc, 2, 64:128] = lower[:64]
            parts[n, dc, 3, 0:64] = upper[64:]
            parts[n, dc, 3, 64:128] = lower[64:]
        far = ys[2]
        for dc in range(2):
            relay_out[n, dc] = parts[n, dc, far].astype(jnp.bfloat16)
            send(relay_out.at[n, dc], relay_in.at[n, dc], relay_send.at[n, dc], relay_recv.at[n, dc],
                 dev_y[dc]).start()

        @pl.when(n == 0)
        def _():
            relay_out[LOW, 0] = low_part(parts[0, 0, far])
            send(relay_out.at[LOW, 0], relay_in.at[LOW, 0], relay_send.at[LOW, 0], relay_recv.at[LOW, 0],
                 dev_y[0]).start()

    def pass_on_low():
        wait_in(relay_in.at[LOW, 0], relay_recv.at[LOW, 0])
        parts[0, 0, y_next] += relay_in[LOW, 0].astype(jnp.float32)
        fin_out[LOW, 0, 0] = low_part(parts[0, 0, y_next] + relay_in[0, 0].astype(jnp.float32))
        fin_out[LOW, 1, 0] = low_part(parts[0, 0, y_prev])
        for way in range(2):
            send(fin_out.at[LOW, way, 0], fin_in.at[LOW, way, 0], fin_send.at[LOW, way], fin_recv.at[LOW, way],
                 dev_y[way]).start()

    def pass_on(n):
        for dc in range(2):
            wait_in(relay_in.at[n, dc], relay_recv.at[n, dc])

        @pl.when(n == 0)
        def _():
            pass_on_low()

        fin_out[n, 0, 0] = (parts[n, 0, y_next] + relay_in[n, 0].astype(jnp.float32)).astype(jnp.bfloat16)
        fin_out[n, 0, 1] = parts[n, 1, y_next].astype(jnp.bfloat16)
        fin_out[n, 1, 0] = parts[n, 0, y_prev].astype(jnp.bfloat16)
        fin_out[n, 1, 1] = (parts[n, 1, y_prev] + relay_in[n, 1].astype(jnp.float32)).astype(jnp.bfloat16)
        for way in range(2):
            send(fin_out.at[n, way], fin_in.at[n, way], fin_send.at[n, way], fin_recv.at[n, way],
                 dev_y[way]).start()

    def cross(n):
        def summed(dc):
            return parts[n, dc, y] + fin_in[n, 0, dc].astype(jnp.float32) + fin_in[n, 1, dc].astype(jnp.float32)

        for way in range(2):
            wait_in(fin_in.at[n, way], fin_recv.at[n, way])

        @pl.when(n == 0)
        def _():
            for way in range(2):
                wait_in(fin_in.at[LOW, way, 0], fin_recv.at[LOW, way])
                parts[0, 0, y] += fin_in[LOW, way, 0].astype(jnp.float32)

            @pl.when(h == 1)
            def _():
                hx_out[LOW] = low_part(summed(0))
                send(hx_out.at[LOW], hx_in.at[LOW], hx_send.at[LOW], hx_recv.at[LOW], dev_h).start()

        hx_out[n] = summed(1 - h).astype(jnp.bfloat16)
        send(hx_out.at[n], hx_in.at[n], hx_send.at[n], hx_recv.at[n], dev_h).start()
        keep[n] = summed(h)

    lane_row = lax.broadcasted_iota(jnp.int32, (1, VB), 1)

    def energies(n, u, dx):
        wait_in(hx_in.at[n], hx_recv.at[n])

        @pl.when(n == 0)
        def _():
            @pl.when(h == 0)
            def _():
                wait_in(hx_in.at[LOW], hx_recv.at[LOW])
                keep[0] += hx_in[LOW].astype(jnp.float32)

        tile = keep[n] + hx_in[n].astype(jnp.float32)
        first = u % 2 * (z - 1)
        second_row = u // 2 * (3 - 3 * (at_least_two - at_three))
        row_z = z * (1 - (u + 1) // 2) + first + second_row
        row_energy = info_in[(row_z - z + 4) % 4 * 2][1:2, :]
        column_energy = info_in[dx * 8 + h][1:2, :]
        denominator = vsum[...] - row_energy - column_energy
        lane = u * 32 + (h * 4 + dx) * 4

        @pl.when(y < 2)
        def _():
            value = -jnp.sum(tile * (2.0 * tile - tile.T) / denominator, axis=0, keepdims=True)
            value = jnp.sum(value, axis=1, keepdims=True)
            acc[0:1, :] += jnp.where(lane_row == lane + 3 * y, value, 0.0)

        @pl.when(y >= 2)
        def _():
            top, bottom, under = tile[:64], tile[64:], denominator[:64]
            value = -jnp.sum(top * (2.0 * top - bottom) / under, axis=0, keepdims=True)
            other = -jnp.sum(bottom * (2.0 * bottom - top) / under, axis=0, keepdims=True)
            value = jnp.sum(value, axis=1, keepdims=True)
            other = jnp.sum(other, axis=1, keepdims=True)
            acc[0:1, :] += jnp.where(lane_row == lane + 1, value, 0.0) + jnp.where(lane_row == lane + 2, other, 0.0)

    def first_arrivals():
        own_x[0].wait_recv()
        passed_x[0].start()
        own_x[2].wait_recv()
        passed_x[1].start()

    def second_arrivals():
        own_x[1].wait_recv()
        core_copy(3).start()
        own_x[3].wait_recv()
        core_copy(1).start()
        wait_in(panels.at[7], d_recv.at[3])
        wait_in(panels.at[5], d_recv.at[1])

        @pl.when(z >= 1)
        def _():
            wait_in(panels.at[8], z_recv.at[1])

    def third_arrivals():
        passed_x[0].wait_recv()
        passed_x[1].wait_recv()
        core_copy(2).start()
        wait_in(panels.at[6], d_recv.at[2])
        for index, (from_z, to_z, u) in enumerate(MOVES):
            if index // 4 == 1:
                @pl.when(z == from_z)
                def _(to_z=to_z, u=u):
                    @pl.when(c == 0)
                    def _():
                        wait_out(panels.at[0], z_send.at[1])
                        pl.semaphore_signal(turn, inc=1, device_id=dev_core, device_id_type=MESH)

                    @pl.when(c == 1)
                    def _():
                        pl.semaphore_wait(turn, 1)
                        z_copy(to_z, u, 1).start()

    def each(low, high, action):
        def one(n, carry):
            action(n)
            return carry

        lax.fori_loop(low, high, one, 0)

    def step(n, carry):
        u_table, dx_table = carry
        products(n, u_table % 4, dx_table % 4)

        @pl.when(n == 0)
        def _():
            pass_on(0)
            first_arrivals()
            cross(0)
            second_arrivals()

        @pl.when(n == second - 1)
        def _():
            each(1, second, pass_on)
            third_arrivals()

        @pl.when(n == third - 1)
        def _():
            each(second, third, pass_on)
            each(1, second, cross)

            @pl.when(z <= 2)
            def _():
                wait_in(panels.at[9], z_recv.at[2])

        return (u_table // 4, dx_table // 4)

    start = jnp.int32(0)
    lax.fori_loop(0, count, step, (start + by_z(U_TABLE), start + by_z(DX_TABLE)))
    each(third, count, pass_on)
    each(second, third, cross)
    wait_in(info_in.at[pl.ds(1, NOCC - 1)], tail_recv.at[0])

    def finish(n, carry):
        u_table, dx_table = carry
        energies(n, u_table % 4, dx_table % 4)
        return (u_table // 4, dx_table // 4)

    tables = lax.fori_loop(0, second, finish, (start + by_z(U_TABLE), start + by_z(DX_TABLE)))
    each(third, count, cross)
    lax.fori_loop(second, count, finish, tables)

    weights = jnp.zeros((1, VB), jnp.float32)
    for k in range(NOCC):
        weights += info_in[k, 0:1, :]
    acc[1:2, :] = acc[0:1, :] * weights
    for _, there, device in plane:
        send(acc, first_in.at[there], tail_send.at[1], tail_recv.at[1], device).start()
    first_in[0] = acc[...]
    wait_in(first_in.at[pl.ds(1, 15)], tail_recv.at[1])
    all_out[5:8, :] = jnp.zeros((3, VB), jnp.float32)
    total = jnp.zeros((1, VB), jnp.float32)
    for kx in range(4):
        both = first_in[4 * kx] + first_in[4 * kx + 1] + first_in[4 * kx + 2] + first_in[4 * kx + 3]
        all_out[kx : kx + 1, :] = both[0:1, :]
        total += both[1:2, :]
    all_out[4:5, :] = total
    for _, there, device in column:
        send(all_out, all_in.at[there], tail_send.at[2], tail_recv.at[2], device).start()
    wanted = codes[...]
    lanes = lax.broadcasted_iota(jnp.int32, (8, VB), 1)
    all_in[0] = all_out[...]

    for k in range(4):
        own_x[k].wait_send()
    for k in range(2):
        passed_x[k].wait_send()
    for dx in range(4):
        core_copy(dx).wait_send()
    wait_out(panels.at[0], z_send.at[0])

    @pl.when(z % 3 == 0)
    def _():
        @pl.when(c == 1)
        def _():
            wait_out(panels.at[0], z_send.at[1])

    def sent(n, carry):
        for k in range(2):
            wait_out(relay_out.at[n, k], relay_send.at[n, k])
            wait_out(fin_out.at[n, k], fin_send.at[n, k])
        wait_out(hx_out.at[n], hx_send.at[n])
        return carry

    lax.fori_loop(0, count, sent, 0)
    wait_out(relay_out.at[LOW, 0], relay_send.at[LOW, 0])
    for way in range(2):
        wait_out(fin_out.at[LOW, way, 0], fin_send.at[LOW, way])

    @pl.when(h == 1)
    def _():
        wait_out(hx_out.at[LOW], hx_send.at[LOW])

    wait_out(info_in.at[pl.ds(1, NOCC - 1)], tail_send.at[0])
    wait_out(first_in.at[pl.ds(1, 15)], tail_send.at[1])

    wait_in(all_in.at[pl.ds(1, 15)], tail_recv.at[2])
    picked = jnp.zeros((8, VB), jnp.float32)
    total = jnp.zeros((1, VB), jnp.float32)
    for kz in range(4):
        for kc in range(2):
            both = all_in[4 * kz + kc] + all_in[4 * kz + 2 + kc]
            total += both[4:5, :]
            for kx in range(4):
                from_row = (xs[kx] * 4 + zs[kz]) * 2 + cs[kc]
                picked += jnp.where(wanted == from_row * VB + lanes, both[kx : kx + 1, :], 0.0)
    sublane = lax.broadcasted_iota(jnp.int32, (8, VB), 0)
    picked = jnp.sum(picked, axis=1, keepdims=True)
    picked = jnp.sum(jnp.where(sublane == lanes, picked, 0.0), axis=0, keepdims=True)
    out[...] = picked[:, : out.shape[1]]
    total_out[...] = jnp.sum(total, axis=1, keepdims=True)
    wait_out(all_in.at[pl.ds(1, 15)], tail_send.at[2])


def place_codes(orbital, table, live):
    partner = jnp.maximum(table[:, 0], 0)
    left = jnp.maximum(table[:, 1], 0)
    right = jnp.maximum(table[:, 2], 0)

    def split(index):
        return index // 8, index // 2 % 4, index % 2

    xi, zi, ci = split(jnp.broadcast_to(orbital, partner.shape))
    xj, zj, cj = split(partner)

    def row_at(first, second):
        found = jnp.full(first.shape, -1, jnp.int32)
        for a in range(4):
            for b in range(4):
                if ROW_AT[a][b] >= 0:
                    found = jnp.where((first == a) & (second == b), ROW_AT[a][b], found)
        return found

    direct = row_at(zi, zj)
    ahead = (xj - xi) % 4
    swap = (direct < 0) | ((zi == zj) & (ahead == 3))
    unit = jnp.where(swap, row_at(zj, zi), direct)
    dx = jnp.where(swap, (4 - ahead) % 4, ahead)
    dc = (ci + cj) % 2
    quadrant = jnp.where(swap, right * 2 + left, left * 2 + right)
    row_x, row_c = jnp.where(swap, xj, xi), jnp.where(swap, cj, ci)
    column_z = jnp.where(swap, zi, zj)
    device = (row_x * 4 + column_z) * 2 + row_c
    lane = unit * 32 + (dc * 4 + dx) * 4 + quadrant
    return jnp.where(live, device * VB + lane, -1)


def local(b_factors, occ_energies, vir_energies, pair_list, pair_count):
    table = pair_list[0]
    slot_total = table.shape[0]
    orbital = lax.axis_index(OCC).astype(jnp.int32)
    share = slot_total // 8
    live = jnp.arange(slot_total, dtype=jnp.int32) < pair_count[0]
    codes = place_codes(orbital, table, live)
    device_hot = (codes[None, :] // VB == jnp.arange(NOCC, dtype=jnp.int32)[:, None]) & live[None, :]
    lane_hot = codes[:, None] % VB == jnp.arange(VB, dtype=jnp.int32)[None, :]
    weights = jnp.dot(device_hot.astype(jnp.bfloat16), lane_hot.astype(jnp.bfloat16),
                      preferred_element_type=jnp.float32)
    sub = lax.broadcasted_iota(jnp.int32, (NOCC, 2, VB), 1)
    info = jnp.where(sub == 0, weights[:, None, :], occ_energies[0])
    mine = lax.dynamic_slice_in_dim(codes, lax.axis_index(AUX) * share, share, 0)
    mine = jnp.concatenate([mine, jnp.full((8 - share,), -1, jnp.int32)])
    mine = jnp.broadcast_to(mine[:, None], (8, VB))
    vmem = pl.BlockSpec(memory_space=pltpu.VMEM)
    bf16, f32 = jnp.bfloat16, jnp.float32
    dma = pltpu.SemaphoreType.DMA
    tile = (VB, VB)
    pair_energy, total_energy = pl.pallas_call(
        kernel,
        out_shape=(jax.ShapeDtypeStruct((1, share), f32), jax.ShapeDtypeStruct((1, 1), f32)),
        in_specs=[pl.BlockSpec(memory_space=pl.ANY), vmem, vmem, vmem],
        out_specs=(vmem, vmem),
        scratch_shapes=[
            pltpu.VMEM((10, *b_factors.shape[1:]), bf16),
            pltpu.VMEM((NOCC, 2, VB), f32),
            pltpu.VMEM((SLOTS, 2, 4, *tile), f32),
            pltpu.VMEM((SLOTS, 2, *tile), bf16),
            pltpu.VMEM((SLOTS, 2, *tile), bf16),
            pltpu.VMEM((SLOTS, 2, 2, *tile), bf16),
            pltpu.VMEM((SLOTS, 2, 2, *tile), bf16),
            pltpu.VMEM((SLOTS, *tile), f32),
            pltpu.VMEM((SLOTS, *tile), bf16),
            pltpu.VMEM((SLOTS, *tile), bf16),
            pltpu.VMEM(tile, f32),
            pltpu.VMEM((2, VB), f32),
            pltpu.VMEM((16, 2, VB), f32),
            pltpu.VMEM((8, VB), f32),
            pltpu.VMEM((16, 8, VB), f32),
            dma, dma((6,)), dma((6,)), dma((4,)), dma((4,)), dma((2,)), dma((3,)),
            dma((SLOTS, 2)), dma((SLOTS, 2)), dma((SLOTS, 2)), dma((SLOTS, 2)),
            dma((SLOTS,)), dma((SLOTS,)), dma((3,)), dma((3,)), pltpu.SemaphoreType.REGULAR,
        ],
        compiler_params=pltpu.CompilerParams(collective_id=0, has_side_effects=True),
        name="pair_energies",
    )(b_factors, info, mine, vir_energies.reshape(2, VB))
    return pair_energy, total_energy[0, 0]


def solution(mesh):
    finer = Mesh(mesh.devices.reshape(4, 4, 2, 4, 2), NAMES)
    placed = (P(OCC, None, AUX), P(OCC), P(), P(OCC, None, None), P(OCC))
    return jax.shard_map(
        local, mesh=finer, in_specs=placed, out_specs=(P(OCC, AUX), P()), check_vma=False
    )
```

```python
import jax
import jax.numpy as jnp
from jax import lax
from jax.experimental import pallas as pl
from jax.experimental.pallas import tpu as pltpu
from jax.sharding import Mesh
from jax.sharding import PartitionSpec as P

VB = 128
NV = 256
NOCC = 32
SLOTS = 12
LOW = SLOTS - 1
HALF = 128
OCC = ("occ_0", "occ_1", "occ_2")
AUX = ("aux_0", "aux_1")
NAMES = ("occ_0", "occ_1", "occ_2", "aux_0", "aux_1")
MESH = pl.DeviceIdType.MESH

UNITS = (
    ((0, 0), (0, 1), (0, 2), (2, 0), (2, 1), (2, 3), (2, 2)),
    ((0, 0), (0, 1), (1, 0), (1, 1), (1, 3), (0, 2), (1, 2), (2, 0), (2, 1), (2, 3), (2, 2)),
    ((0, 0), (0, 1), (1, 0), (1, 1), (1, 3), (0, 2), (1, 2), (2, 0), (2, 1), (2, 3), (2, 2)),
    ((0, 0), (0, 1), (1, 0), (1, 1), (1, 3), (0, 2), (1, 2)),
)
COUNT = (7, 11, 11, 7)
SECOND = (2, 5, 5, 5)
THIRD = (3, 7, 7, 7)
MOVES = ((0, 1, 1), (1, 2, 1), (2, 3, 1), (3, 1, 2), (0, 2, 2), (3, 0, 2))
ROW_AT = ((0, 1, 2, -1), (-1, 0, 1, -1), (-1, -1, 0, 1), (2, 2, -1, 0))


def packed(values):
    total = 0
    for place, value in enumerate(values):
        total += value * 4**place
    return total


U_TABLE = tuple(packed([u for u, _ in row]) for row in UNITS)
DX_TABLE = tuple(packed([dx for _, dx in row]) for row in UNITS)


def place_codes(x, z, c, partner, left, right, live):
    partner, left, right = (jnp.maximum(v, 0) for v in (partner, left, right))
    xj, zj, cj = partner >> 3, (partner >> 1) & 3, partner & 1
    xi, zi, ci = (jnp.full(partner.shape, v, jnp.int32) for v in (x, z, c))

    def row_at(first, second):
        key = first * 4 + second
        found = jnp.full(key.shape, -1, jnp.int32)
        for a in range(4):
            for b in range(4):
                if ROW_AT[a][b] >= 0:
                    found = jnp.where(key == a * 4 + b, ROW_AT[a][b], found)
        return found

    direct = row_at(zi, zj)
    ahead = (xj - xi) & 3
    swap = (direct < 0) | ((zi == zj) & (ahead == 3))
    unit = jnp.where(swap, row_at(zj, zi), direct)
    dx = jnp.where(swap, (4 - ahead) & 3, ahead)
    dc = (ci + cj) & 1
    quadrant = jnp.where(swap, right * 2 + left, left * 2 + right)
    device = (jnp.where(swap, xj, xi) * 4 + jnp.where(swap, zi, zj)) * 2 + jnp.where(swap, cj, ci)
    lane = unit * 32 + (dc * 4 + dx) * 4 + quadrant
    return jnp.where(live, device * VB + lane, -1)


def kernel(b_hbm, energy, items, listed, vir, out, total_out, panels, info_out, info_in, parts, relay_out, relay_in, fin_out, fin_in,
           keep, hx_out, hx_in, vsum, acc, first_in, all_out, all_in,
           load_sem, x_send, x_recv, d_send, d_recv, z_send, z_recv, relay_send, relay_recv,
           fin_send, fin_recv, hx_send, hx_recv, tail_send, tail_recv, turn, calm):
    x, z, c, y, h = (lax.axis_index(name) for name in NAMES)
    me = (x * 4 + z) * 2 + c
    xs, zs, ys = ([(v + k) % 4 for k in range(4)] for v in (x, z, y))
    cs, hs = (c, 1 - c), (h, 1 - h)
    at_least_one = (z + 3) // 4
    at_least_two = z // 2
    at_three = z // 3

    def by_z(table):
        steps = [table[k + 1] - table[k] for k in range(3)]
        return table[0] + steps[0] * at_least_one + steps[1] * at_least_two + steps[2] * at_three

    x_next, x_prev, y_next, y_prev = xs[1], xs[3], ys[1], ys[3]
    dev_x = ((x_next, z, c, y, h), (x_prev, z, c, y, h))
    dev_y = ((x, z, c, y_next, h), (x, z, c, y_prev, h))
    dev_core = (x, z, 1 - c, y, h)
    dev_h = (x, z, c, y, 1 - h)

    others = []
    for k in range(1, NOCC):
        kx, kz, kc = k // 8, k // 2 % 4, k % 2
        there = (-kx % 4 * 4 + -kz % 4) * 2 + kc
        others.append((k, there, (xs[kx], zs[kz], cs[kc], y, h), (xs[kx] * 4 + zs[kz]) * 2 + cs[kc]))
    plane = [(k, -(k // 4) % 4 * 4 + -k % 4, (xs[k // 4], z, c, ys[k % 4], h)) for k in range(1, 16)]
    column = [(k, (-(k // 4) % 4 * 2 + k // 2 % 2) * 2 + k % 2, (x, zs[k // 4], cs[k % 2], y, hs[k // 2 % 2]))
              for k in range(1, 16)]
    greeted = [device for _, _, device, _ in others] + [dev_h]
    greeted += [device for k, _, device in plane if k % 4 != 0]
    greeted += [device for k, _, device in column if k // 2 % 2 == 1 and k != 2]

    def send(src, dst, send_sem, recv_sem, device):
        return pltpu.make_async_remote_copy(
            src_ref=src, dst_ref=dst, send_sem=send_sem, recv_sem=recv_sem,
            device_id=device, device_id_type=MESH)

    def wait_in(dst, recv_sem):
        send(dst, dst, x_send.at[0], recv_sem, dev_core).wait_recv()

    def wait_out(src, send_sem):
        send(src, src, send_sem, x_recv.at[0], dev_core).wait_send()

    def half(slot, part):
        return panels.at[slot, pl.ds(part * HALF, HALF)]

    load = pltpu.make_async_copy(b_hbm.at[0], panels.at[0], load_sem)
    load.start()

    barrier = pltpu.get_barrier_semaphore()

    for device in greeted:
        pl.semaphore_signal(barrier, inc=1, device_id=device, device_id_type=MESH)
    load.wait()
    pl.semaphore_wait(barrier, len(greeted))

    own_x = (
        send(half(0, 0), half(3, 0), x_send.at[0], x_recv.at[0], dev_x[0]),
        send(half(0, 1), half(3, 1), x_send.at[1], x_recv.at[1], dev_x[0]),
        send(half(0, 1), half(1, 1), x_send.at[2], x_recv.at[2], dev_x[1]),
        send(half(0, 0), half(1, 0), x_send.at[3], x_recv.at[3], dev_x[1]),
    )
    passed_x = (
        send(half(3, 0), half(2, 0), x_send.at[4], x_recv.at[4], dev_x[0]),
        send(half(1, 1), half(2, 1), x_send.at[5], x_recv.at[5], dev_x[1]),
    )

    def core_copy(dx):
        return send(panels.at[dx], panels.at[4 + dx], d_send.at[dx], d_recv.at[dx], dev_core)

    def z_copy(to_z, u, kind):
        return send(panels.at[0], panels.at[7 + u], z_send.at[kind], z_recv.at[u], (x, to_z, c, y, h))

    own_x[0].start()
    own_x[2].start()
    for index, (from_z, to_z, u) in enumerate(MOVES):
        @pl.when(z == from_z)
        def _(to_z=to_z, u=u, kind=index // 4):
            if kind == 0:
                z_copy(to_z, u, kind).start()
            else:
                @pl.when(c == 0)
                def _():
                    z_copy(to_z, u, kind).start()

    core_copy(0).start()
    own_x[1].start()
    own_x[3].start()

    slots = items.shape[2]
    slot_of = lax.broadcasted_iota(jnp.int32, (1, slots), 1)
    codes = place_codes(x, z, c, items[0], items[1], items[2], slot_of < listed[...])
    device_hot = lax.broadcasted_iota(jnp.int32, (NOCC, slots), 0) == codes >> 7
    lane_hot = (lax.broadcasted_iota(jnp.int32, (VB, slots), 0) == codes & (VB - 1)) & (codes >= 0)
    hits = lax.dot_general(device_hot.astype(jnp.float32).astype(jnp.bfloat16),
                           lane_hot.astype(jnp.float32).astype(jnp.bfloat16),
                           (((1,), (1,)), ((), ())), preferred_element_type=jnp.float32)
    for k in range(NOCC):
        info_out[k, 0:1, :] = hits[k : k + 1, :]
        info_out[k, 1:2, :] = jnp.broadcast_to(energy[...], (1, VB))
    share = out.shape[1]
    sublane = lax.broadcasted_iota(jnp.int32, (8, slots), 0)
    mine = lax.broadcasted_iota(jnp.int32, (8, slots), 1) == (y * 2 + h) * share + sublane
    wanted = jnp.max(jnp.where(mine & (sublane < share), codes, -1), axis=1, keepdims=True)

    for _, there, device, index in others:
        send(info_out.at[index], info_in.at[there], tail_send.at[0], tail_recv.at[0], device).start()
    info_in[0] = info_out[me]
    acc[...] = jnp.zeros_like(acc)

    wait_in(panels.at[4], d_recv.at[0])

    row_of = lax.broadcasted_iota(jnp.int32, (VB, VB), 0)
    lane_of = lax.broadcasted_iota(jnp.int32, (VB, VB), 1)
    left = vir[0]
    right = vir[1]

    def as_column(row_values, shift):
        wide = jnp.broadcast_to(row_values, (VB, VB))
        return jnp.sum(jnp.where(lane_of == shift, wide, 0.0), axis=1, keepdims=True)

    @pl.when(y == 0)
    def _():
        vsum[...] = as_column(left, row_of) + left

    @pl.when(y == 1)
    def _():
        vsum[...] = as_column(right, row_of) + right

    @pl.when(y == 2)
    def _():
        vsum[...] = as_column(left, row_of % 64) + right

    @pl.when(y == 3)
    def _():
        vsum[...] = as_column(left, row_of % 64 + 64) + right

    count = by_z(COUNT)
    second = by_z(SECOND)
    third = by_z(THIRD)

    def low_part(value):
        return (value - value.astype(jnp.bfloat16).astype(jnp.float32)).astype(jnp.bfloat16)

    def products(n, u, dx):
        row_slot = (7 + u) * ((u + 3) // 4)
        rows = panels[row_slot]
        for dc in range(2):
            block = lax.dot_general(rows, panels[dc * 4 + dx], (((1,), (1,)), ((), ())),
                                    preferred_element_type=jnp.float32)
            upper = block[:VB, VB:]
            lower = block[VB:, :VB].T
            parts[n, dc, 0] = block[:VB, :VB]
            parts[n, dc, 1] = block[VB:, VB:]
            parts[n, dc, 2, 0:64] = upper[:64]
            parts[n, dc, 2, 64:128] = lower[:64]
            parts[n, dc, 3, 0:64] = upper[64:]
            parts[n, dc, 3, 64:128] = lower[64:]
        far = ys[2]
        for dc in range(2):
            relay_out[n, dc] = parts[n, dc, far].astype(jnp.bfloat16)
            send(relay_out.at[n, dc], relay_in.at[n, dc], relay_send.at[n, dc], relay_recv.at[n, dc],
                 dev_y[dc]).start()

        @pl.when(n == 0)
        def _():
            relay_out[LOW, 0] = low_part(parts[0, 0, far])
            send(relay_out.at[LOW, 0], relay_in.at[LOW, 0], relay_send.at[LOW, 0], relay_recv.at[LOW, 0],
                 dev_y[0]).start()

    def pass_on_low():
        wait_in(relay_in.at[LOW, 0], relay_recv.at[LOW, 0])
        parts[0, 0, y_next] += relay_in[LOW, 0].astype(jnp.float32)
        fin_out[LOW, 0, 0] = low_part(parts[0, 0, y_next] + relay_in[0, 0].astype(jnp.float32))
        fin_out[LOW, 1, 0] = low_part(parts[0, 0, y_prev])
        for way in range(2):
            send(fin_out.at[LOW, way, 0], fin_in.at[LOW, way, 0], fin_send.at[LOW, way], fin_recv.at[LOW, way],
                 dev_y[way]).start()

    def pass_on(n):
        for dc in range(2):
            wait_in(relay_in.at[n, dc], relay_recv.at[n, dc])

        @pl.when(n == 0)
        def _():
            pass_on_low()

        fin_out[n, 0, 0] = (parts[n, 0, y_next] + relay_in[n, 0].astype(jnp.float32)).astype(jnp.bfloat16)
        fin_out[n, 0, 1] = parts[n, 1, y_next].astype(jnp.bfloat16)
        fin_out[n, 1, 0] = parts[n, 0, y_prev].astype(jnp.bfloat16)
        fin_out[n, 1, 1] = (parts[n, 1, y_prev] + relay_in[n, 1].astype(jnp.float32)).astype(jnp.bfloat16)
        for way in range(2):
            send(fin_out.at[n, way], fin_in.at[n, way], fin_send.at[n, way], fin_recv.at[n, way],
                 dev_y[way]).start()

    def cross(n):
        def summed(dc):
            return parts[n, dc, y] + fin_in[n, 0, dc].astype(jnp.float32) + fin_in[n, 1, dc].astype(jnp.float32)

        for way in range(2):
            wait_in(fin_in.at[n, way], fin_recv.at[n, way])

        @pl.when(n == 0)
        def _():
            for way in range(2):
                wait_in(fin_in.at[LOW, way, 0], fin_recv.at[LOW, way])
                parts[0, 0, y] += fin_in[LOW, way, 0].astype(jnp.float32)

            @pl.when(h == 1)
            def _():
                hx_out[LOW] = low_part(summed(0))
                send(hx_out.at[LOW], hx_in.at[LOW], hx_send.at[LOW], hx_recv.at[LOW], dev_h).start()

        hx_out[n] = summed(1 - h).astype(jnp.bfloat16)
        send(hx_out.at[n], hx_in.at[n], hx_send.at[n], hx_recv.at[n], dev_h).start()
        keep[n] = summed(h)

    lane_row = lax.broadcasted_iota(jnp.int32, (1, VB), 1)

    def energies(n, u, dx):
        wait_in(hx_in.at[n], hx_recv.at[n])

        @pl.when(n == 0)
        def _():
            @pl.when(h == 0)
            def _():
                wait_in(hx_in.at[LOW], hx_recv.at[LOW])
                keep[0] += hx_in[LOW].astype(jnp.float32)

        tile = keep[n] + hx_in[n].astype(jnp.float32)
        first = u % 2 * (z - 1)
        second_row = u // 2 * (3 - 3 * (at_least_two - at_three))
        row_z = z * (1 - (u + 1) // 2) + first + second_row
        row_energy = info_in[(row_z - z + 4) % 4 * 2][1:2, :]
        column_energy = info_in[dx * 8 + h][1:2, :]
        denominator = vsum[...] - row_energy - column_energy
        lane = u * 32 + (h * 4 + dx) * 4

        @pl.when(y < 2)
        def _():
            value = -jnp.sum(tile * (2.0 * tile - tile.T) / denominator, axis=0, keepdims=True)
            value = jnp.sum(value, axis=1, keepdims=True)
            acc[0:1, :] += jnp.where(lane_row == lane + 3 * y, value, 0.0)

        @pl.when(y >= 2)
        def _():
            top, bottom, under = tile[:64], tile[64:], denominator[:64]
            value = -jnp.sum(top * (2.0 * top - bottom) / under, axis=0, keepdims=True)
            other = -jnp.sum(bottom * (2.0 * bottom - top) / under, axis=0, keepdims=True)
            value = jnp.sum(value, axis=1, keepdims=True)
            other = jnp.sum(other, axis=1, keepdims=True)
            acc[0:1, :] += jnp.where(lane_row == lane + 1, value, 0.0) + jnp.where(lane_row == lane + 2, other, 0.0)

    def first_arrivals():
        own_x[0].wait_recv()
        passed_x[0].start()
        own_x[2].wait_recv()
        passed_x[1].start()

    def second_arrivals():
        own_x[1].wait_recv()
        core_copy(3).start()
        own_x[3].wait_recv()
        core_copy(1).start()
        wait_in(panels.at[7], d_recv.at[3])
        wait_in(panels.at[5], d_recv.at[1])

        @pl.when(z >= 1)
        def _():
            wait_in(panels.at[8], z_recv.at[1])

    def third_arrivals():
        passed_x[0].wait_recv()
        passed_x[1].wait_recv()
        core_copy(2).start()
        wait_in(panels.at[6], d_recv.at[2])
        for index, (from_z, to_z, u) in enumerate(MOVES):
            if index // 4 == 1:
                @pl.when(z == from_z)
                def _(to_z=to_z, u=u):
                    @pl.when(c == 0)
                    def _():
                        wait_out(panels.at[0], z_send.at[1])
                        pl.semaphore_signal(turn, inc=1, device_id=dev_core, device_id_type=MESH)

                    @pl.when(c == 1)
                    def _():
                        pl.semaphore_wait(turn, 1)
                        z_copy(to_z, u, 1).start()

    def each(low, high, action):
        def one(n, carry):
            action(n)
            return carry

        lax.fori_loop(low, high, one, 0)

    def step(n, carry):
        u_table, dx_table = carry
        products(n, u_table % 4, dx_table % 4)

        @pl.when(n == 0)
        def _():
            pass_on(0)
            first_arrivals()
            cross(0)
            second_arrivals()

        @pl.when(n == second - 1)
        def _():
            each(1, second, pass_on)
            third_arrivals()

        @pl.when(n == third - 1)
        def _():
            each(second, third, pass_on)

            @pl.when(z <= 2)
            def _():
                wait_in(panels.at[9], z_recv.at[2])

            @pl.when(z == 2)
            def _():
                for to_z in (1, 3):
                    pl.semaphore_signal(calm, inc=1, device_id=(x, to_z, c, y, h), device_id_type=MESH)

        return (u_table // 4, dx_table // 4)

    start = jnp.int32(0)
    lax.fori_loop(0, count, step, (start + by_z(U_TABLE), start + by_z(DX_TABLE)))

    @pl.when(z % 2 == 1)
    def _():
        pl.semaphore_wait(calm, 1)

    each(1, third, cross)
    each(third, count, pass_on)
    wait_in(info_in.at[pl.ds(1, NOCC - 1)], tail_recv.at[0])

    def finish(n, carry):
        u_table, dx_table = carry
        energies(n, u_table % 4, dx_table % 4)
        return (u_table // 4, dx_table // 4)

    each(third, count, cross)
    lax.fori_loop(0, count, finish, (start + by_z(U_TABLE), start + by_z(DX_TABLE)))

    weights = jnp.zeros((1, VB), jnp.float32)
    for k in range(NOCC):
        weights += info_in[k, 0:1, :]
    acc[1:2, :] = acc[0:1, :] * weights
    for _, there, device in plane:
        send(acc, first_in.at[there], tail_send.at[1], tail_recv.at[1], device).start()
    first_in[0] = acc[...]
    wait_in(first_in.at[pl.ds(1, 15)], tail_recv.at[1])
    all_out[5:8, :] = jnp.zeros((3, VB), jnp.float32)
    total = jnp.zeros((1, VB), jnp.float32)
    for kx in range(4):
        both = first_in[4 * kx] + first_in[4 * kx + 1] + first_in[4 * kx + 2] + first_in[4 * kx + 3]
        all_out[kx : kx + 1, :] = both[0:1, :]
        total += both[1:2, :]
    all_out[4:5, :] = total
    for _, there, device in column:
        send(all_out, all_in.at[there], tail_send.at[2], tail_recv.at[2], device).start()
    lanes = lax.broadcasted_iota(jnp.int32, (8, VB), 1)
    all_in[0] = all_out[...]

    for k in range(4):
        own_x[k].wait_send()
    for k in range(2):
        passed_x[k].wait_send()
    for dx in range(4):
        core_copy(dx).wait_send()
    wait_out(panels.at[0], z_send.at[0])

    @pl.when(z % 3 == 0)
    def _():
        @pl.when(c == 1)
        def _():
            wait_out(panels.at[0], z_send.at[1])

    def sent(n, carry):
        for k in range(2):
            wait_out(relay_out.at[n, k], relay_send.at[n, k])
            wait_out(fin_out.at[n, k], fin_send.at[n, k])
        wait_out(hx_out.at[n], hx_send.at[n])
        return carry

    lax.fori_loop(0, count, sent, 0)
    wait_out(relay_out.at[LOW, 0], relay_send.at[LOW, 0])
    for way in range(2):
        wait_out(fin_out.at[LOW, way, 0], fin_send.at[LOW, way])

    @pl.when(h == 1)
    def _():
        wait_out(hx_out.at[LOW], hx_send.at[LOW])

    wait_out(info_in.at[pl.ds(1, NOCC - 1)], tail_send.at[0])
    wait_out(first_in.at[pl.ds(1, 15)], tail_send.at[1])

    wait_in(all_in.at[pl.ds(1, 15)], tail_recv.at[2])
    picked = jnp.zeros((8, VB), jnp.float32)
    total = jnp.zeros((1, VB), jnp.float32)
    for kz in range(4):
        for kc in range(2):
            both = all_in[4 * kz + kc] + all_in[4 * kz + 2 + kc]
            total += both[4:5, :]
            for kx in range(4):
                from_row = (xs[kx] * 4 + zs[kz]) * 2 + cs[kc]
                picked += jnp.where(jnp.broadcast_to(wanted, (8, VB)) == from_row * VB + lanes, both[kx : kx + 1, :], 0.0)
    sublane = lax.broadcasted_iota(jnp.int32, (8, VB), 0)
    picked = jnp.sum(picked, axis=1, keepdims=True)
    picked = jnp.sum(jnp.where(sublane == lanes, picked, 0.0), axis=0, keepdims=True)
    out[...] = picked[:, : out.shape[1]]
    total_out[...] = jnp.sum(total, axis=1, keepdims=True)
    wait_out(all_in.at[pl.ds(1, 15)], tail_send.at[2])


def local(b_factors, occ_energies, vir_energies, pair_list, pair_count):
    slot_total = pair_list.shape[1]
    share = slot_total // 8
    vmem = pl.BlockSpec(memory_space=pltpu.VMEM)
    bf16, f32 = jnp.bfloat16, jnp.float32
    dma = pltpu.SemaphoreType.DMA
    tile = (VB, VB)
    pair_energy, total_energy = pl.pallas_call(
        kernel,
        out_shape=(jax.ShapeDtypeStruct((1, share), f32), jax.ShapeDtypeStruct((1, 1), f32)),
        in_specs=[pl.BlockSpec(memory_space=pl.ANY), vmem, vmem, vmem, vmem],
        out_specs=(vmem, vmem),
        scratch_shapes=[
            pltpu.VMEM((10, *b_factors.shape[1:]), bf16),
            pltpu.VMEM((NOCC, 2, VB), f32),
            pltpu.VMEM((NOCC, 2, VB), f32),
            pltpu.VMEM((SLOTS, 2, 4, *tile), f32),
            pltpu.VMEM((SLOTS, 2, *tile), bf16),
            pltpu.VMEM((SLOTS, 2, *tile), bf16),
            pltpu.VMEM((SLOTS, 2, 2, *tile), bf16),
            pltpu.VMEM((SLOTS, 2, 2, *tile), bf16),
            pltpu.VMEM((SLOTS, *tile), f32),
            pltpu.VMEM((SLOTS, *tile), bf16),
            pltpu.VMEM((SLOTS, *tile), bf16),
            pltpu.VMEM(tile, f32),
            pltpu.VMEM((2, VB), f32),
            pltpu.VMEM((16, 2, VB), f32),
            pltpu.VMEM((8, VB), f32),
            pltpu.VMEM((16, 8, VB), f32),
            dma, dma((6,)), dma((6,)), dma((4,)), dma((4,)), dma((2,)), dma((3,)),
            dma((SLOTS, 2)), dma((SLOTS, 2)), dma((SLOTS, 2)), dma((SLOTS, 2)),
            dma((SLOTS,)), dma((SLOTS,)), dma((3,)), dma((3,)), pltpu.SemaphoreType.REGULAR,
            pltpu.SemaphoreType.REGULAR,
        ],
        compiler_params=pltpu.CompilerParams(collective_id=0, has_side_effects=True),
        name="pair_energies",
    )(b_factors, occ_energies.reshape(1, 1), jnp.transpose(pair_list, (2, 0, 1)), pair_count.reshape(1, 1),
      vir_energies.reshape(2, 1, VB))
    return pair_energy, total_energy[0, 0]


def solution(mesh):
    finer = Mesh(mesh.devices.reshape(4, 4, 2, 4, 2), NAMES)
    placed = (P(OCC, None, AUX), P(OCC), P(), P(OCC, None, None), P(OCC))
    return jax.shard_map(
        local, mesh=finer, in_specs=placed, out_specs=(P(OCC, AUX), P()), check_vma=False
    )
```

```python
import jax
import jax.numpy as jnp
from jax import lax
from jax.experimental import pallas as pl
from jax.experimental.pallas import tpu as pltpu
from jax.sharding import Mesh
from jax.sharding import PartitionSpec as P

VB = 128
NV = 256
NOCC = 32
SLOTS = 12
LOW = SLOTS - 1
HALF = 128
OCC = ("occ_0", "occ_1", "occ_2")
AUX = ("aux_0", "aux_1")
NAMES = ("occ_0", "occ_1", "occ_2", "aux_0", "aux_1")
MESH = pl.DeviceIdType.MESH

UNITS = (
    ((0, 0), (0, 1), (0, 2), (2, 0), (2, 1), (2, 3), (2, 2)),
    ((0, 0), (0, 1), (1, 0), (1, 1), (1, 3), (0, 2), (1, 2), (2, 0), (2, 1), (2, 3), (2, 2)),
    ((0, 0), (0, 1), (1, 0), (1, 1), (1, 3), (0, 2), (1, 2), (2, 0), (2, 1), (2, 3), (2, 2)),
    ((0, 0), (0, 1), (1, 0), (1, 1), (1, 3), (0, 2), (1, 2)),
)
COUNT = (7, 11, 11, 7)
SECOND = (2, 5, 5, 5)
THIRD = (3, 7, 7, 7)
MOVES = ((0, 1, 1), (1, 2, 1), (2, 3, 1), (3, 1, 2), (0, 2, 2), (3, 0, 2))
ROW_AT = ((0, 1, 2, -1), (-1, 0, 1, -1), (-1, -1, 0, 1), (2, 2, -1, 0))


def packed(values):
    total = 0
    for place, value in enumerate(values):
        total += value * 4**place
    return total


U_TABLE = tuple(packed([u for u, _ in row]) for row in UNITS)
DX_TABLE = tuple(packed([dx for _, dx in row]) for row in UNITS)


def place_codes(x, z, c, partner, left, right, live):
    partner, left, right = (jnp.maximum(v, 0) for v in (partner, left, right))
    xj, zj, cj = partner >> 3, (partner >> 1) & 3, partner & 1
    xi, zi, ci = (jnp.full(partner.shape, v, jnp.int32) for v in (x, z, c))

    def row_at(first, second):
        key = first * 4 + second
        found = jnp.full(key.shape, -1, jnp.int32)
        for a in range(4):
            for b in range(4):
                if ROW_AT[a][b] >= 0:
                    found = jnp.where(key == a * 4 + b, ROW_AT[a][b], found)
        return found

    direct = row_at(zi, zj)
    ahead = (xj - xi) & 3
    swap = (direct < 0) | ((zi == zj) & (ahead == 3))
    unit = jnp.where(swap, row_at(zj, zi), direct)
    dx = jnp.where(swap, (4 - ahead) & 3, ahead)
    dc = (ci + cj) & 1
    quadrant = jnp.where(swap, right * 2 + left, left * 2 + right)
    device = (jnp.where(swap, xj, xi) * 4 + jnp.where(swap, zi, zj)) * 2 + jnp.where(swap, cj, ci)
    lane = unit * 32 + (dc * 4 + dx) * 4 + quadrant
    return jnp.where(live, device * VB + lane, -1)


def kernel(b_hbm, energy, items, listed, vir, out, total_out, panels, info_out, info_in, parts, relay_out, relay_in, fin_out, fin_in,
           keep, hx_out, hx_in, vsum, acc, first_in, all_out, all_in,
           load_sem, x_send, x_recv, d_send, d_recv, z_send, z_recv, relay_send, relay_recv,
           fin_send, fin_recv, hx_send, hx_recv, tail_send, tail_recv, turn, calm):
    x, z, c, y, h = (lax.axis_index(name) for name in NAMES)
    me = (x * 4 + z) * 2 + c
    xs, zs, ys = ([(v + k) % 4 for k in range(4)] for v in (x, z, y))
    cs, hs = (c, 1 - c), (h, 1 - h)
    at_least_one = (z + 3) // 4
    at_least_two = z // 2
    at_three = z // 3

    def by_z(table):
        steps = [table[k + 1] - table[k] for k in range(3)]
        return table[0] + steps[0] * at_least_one + steps[1] * at_least_two + steps[2] * at_three

    x_next, x_prev, y_next, y_prev = xs[1], xs[3], ys[1], ys[3]
    dev_x = ((x_next, z, c, y, h), (x_prev, z, c, y, h))
    dev_y = ((x, z, c, y_next, h), (x, z, c, y_prev, h))
    dev_core = (x, z, 1 - c, y, h)
    dev_h = (x, z, c, y, 1 - h)

    others = []
    for k in range(1, NOCC):
        kx, kz, kc = k // 8, k // 2 % 4, k % 2
        there = (-kx % 4 * 4 + -kz % 4) * 2 + kc
        others.append((k, there, (xs[kx], zs[kz], cs[kc], y, h), (xs[kx] * 4 + zs[kz]) * 2 + cs[kc]))
    plane = [(k, -(k // 4) % 4 * 4 + -k % 4, (xs[k // 4], z, c, ys[k % 4], h)) for k in range(1, 16)]
    column = [(k, (-(k // 4) % 4 * 2 + k // 2 % 2) * 2 + k % 2, (x, zs[k // 4], cs[k % 2], y, hs[k // 2 % 2]))
              for k in range(1, 16)]
    greeted = [device for _, _, device, _ in others] + [dev_h]
    greeted += [device for k, _, device in plane if k % 4 != 0]
    greeted += [device for k, _, device in column if k // 2 % 2 == 1 and k != 2]

    def send(src, dst, send_sem, recv_sem, device):
        return pltpu.make_async_remote_copy(
            src_ref=src, dst_ref=dst, send_sem=send_sem, recv_sem=recv_sem,
            device_id=device, device_id_type=MESH)

    def wait_in(dst, recv_sem):
        send(dst, dst, x_send.at[0], recv_sem, dev_core).wait_recv()

    def wait_out(src, send_sem):
        send(src, src, send_sem, x_recv.at[0], dev_core).wait_send()

    def half(slot, part):
        return panels.at[slot, pl.ds(part * HALF, HALF)]

    load = pltpu.make_async_copy(b_hbm.at[0], panels.at[0], load_sem)
    load.start()

    barrier = pltpu.get_barrier_semaphore()

    for device in reversed(greeted):
        pl.semaphore_signal(barrier, inc=1, device_id=device, device_id_type=MESH)
    load.wait()
    pl.semaphore_wait(barrier, len(greeted))

    own_x = (
        send(half(0, 0), half(3, 0), x_send.at[0], x_recv.at[0], dev_x[0]),
        send(half(0, 1), half(3, 1), x_send.at[1], x_recv.at[1], dev_x[0]),
        send(half(0, 1), half(1, 1), x_send.at[2], x_recv.at[2], dev_x[1]),
        send(half(0, 0), half(1, 0), x_send.at[3], x_recv.at[3], dev_x[1]),
    )
    passed_x = (
        send(half(3, 0), half(2, 0), x_send.at[4], x_recv.at[4], dev_x[0]),
        send(half(1, 1), half(2, 1), x_send.at[5], x_recv.at[5], dev_x[1]),
    )

    def core_copy(dx):
        return send(panels.at[dx], panels.at[4 + dx], d_send.at[dx], d_recv.at[dx], dev_core)

    def z_copy(to_z, u, kind):
        return send(panels.at[0], panels.at[7 + u], z_send.at[kind], z_recv.at[u], (x, to_z, c, y, h))

    for index, (from_z, to_z, u) in enumerate(MOVES):
        @pl.when(z == from_z)
        def _(to_z=to_z, u=u, kind=index // 4):
            if kind == 0:
                z_copy(to_z, u, kind).start()
            else:
                @pl.when(c == 0)
                def _():
                    z_copy(to_z, u, kind).start()

    own_x[0].start()
    own_x[2].start()
    core_copy(0).start()
    own_x[1].start()
    own_x[3].start()

    slots = items.shape[2]
    slot_of = lax.broadcasted_iota(jnp.int32, (1, slots), 1)
    codes = place_codes(x, z, c, items[0], items[1], items[2], slot_of < listed[...])
    device_hot = lax.broadcasted_iota(jnp.int32, (NOCC, slots), 0) == codes >> 7
    lane_hot = (lax.broadcasted_iota(jnp.int32, (VB, slots), 0) == codes & (VB - 1)) & (codes >= 0)
    hits = lax.dot_general(device_hot.astype(jnp.float32).astype(jnp.bfloat16),
                           lane_hot.astype(jnp.float32).astype(jnp.bfloat16),
                           (((1,), (1,)), ((), ())), preferred_element_type=jnp.float32)
    for k in range(NOCC):
        info_out[k, 0:1, :] = hits[k : k + 1, :]
        info_out[k, 1:2, :] = jnp.broadcast_to(energy[...], (1, VB))
    share = out.shape[1]
    sublane = lax.broadcasted_iota(jnp.int32, (8, slots), 0)
    mine = lax.broadcasted_iota(jnp.int32, (8, slots), 1) == (y * 2 + h) * share + sublane
    wanted = jnp.max(jnp.where(mine & (sublane < share), codes, -1), axis=1, keepdims=True)

    for _, there, device, index in others:
        send(info_out.at[index], info_in.at[there], tail_send.at[0], tail_recv.at[0], device).start()
    info_in[0] = info_out[me]
    acc[...] = jnp.zeros_like(acc)

    wait_in(panels.at[4], d_recv.at[0])

    row_of = lax.broadcasted_iota(jnp.int32, (VB, VB), 0)
    lane_of = lax.broadcasted_iota(jnp.int32, (VB, VB), 1)
    left = vir[0]
    right = vir[1]

    def as_column(row_values, shift):
        wide = jnp.broadcast_to(row_values, (VB, VB))
        return jnp.sum(jnp.where(lane_of == shift, wide, 0.0), axis=1, keepdims=True)

    @pl.when(y == 0)
    def _():
        vsum[...] = as_column(left, row_of) + left

    @pl.when(y == 1)
    def _():
        vsum[...] = as_column(right, row_of) + right

    @pl.when(y == 2)
    def _():
        vsum[...] = as_column(left, row_of % 64) + right

    @pl.when(y == 3)
    def _():
        vsum[...] = as_column(left, row_of % 64 + 64) + right

    count = by_z(COUNT)
    second = by_z(SECOND)
    third = by_z(THIRD)

    def low_part(value):
        return (value - value.astype(jnp.bfloat16).astype(jnp.float32)).astype(jnp.bfloat16)

    def products(n, u, dx):
        row_slot = (7 + u) * ((u + 3) // 4)
        rows = panels[row_slot]
        for dc in range(2):
            block = lax.dot_general(rows, panels[dc * 4 + dx], (((1,), (1,)), ((), ())),
                                    preferred_element_type=jnp.float32)
            upper = block[:VB, VB:]
            lower = block[VB:, :VB].T
            parts[n, dc, 0] = block[:VB, :VB]
            parts[n, dc, 1] = block[VB:, VB:]
            parts[n, dc, 2, 0:64] = upper[:64]
            parts[n, dc, 2, 64:128] = lower[:64]
            parts[n, dc, 3, 0:64] = upper[64:]
            parts[n, dc, 3, 64:128] = lower[64:]
        far = ys[2]
        for dc in range(2):
            relay_out[n, dc] = parts[n, dc, far].astype(jnp.bfloat16)
            send(relay_out.at[n, dc], relay_in.at[n, dc], relay_send.at[n, dc], relay_recv.at[n, dc],
                 dev_y[dc]).start()

        @pl.when(n == 0)
        def _():
            relay_out[LOW, 0] = low_part(parts[0, 0, far])
            send(relay_out.at[LOW, 0], relay_in.at[LOW, 0], relay_send.at[LOW, 0], relay_recv.at[LOW, 0],
                 dev_y[0]).start()

    def pass_on_low():
        wait_in(relay_in.at[LOW, 0], relay_recv.at[LOW, 0])
        parts[0, 0, y_next] += relay_in[LOW, 0].astype(jnp.float32)
        fin_out[LOW, 0, 0] = low_part(parts[0, 0, y_next] + relay_in[0, 0].astype(jnp.float32))
        fin_out[LOW, 1, 0] = low_part(parts[0, 0, y_prev])
        for way in range(2):
            send(fin_out.at[LOW, way, 0], fin_in.at[LOW, way, 0], fin_send.at[LOW, way], fin_recv.at[LOW, way],
                 dev_y[way]).start()

    def pass_on(n):
        for dc in range(2):
            wait_in(relay_in.at[n, dc], relay_recv.at[n, dc])

        @pl.when(n == 0)
        def _():
            pass_on_low()

        fin_out[n, 0, 0] = (parts[n, 0, y_next] + relay_in[n, 0].astype(jnp.float32)).astype(jnp.bfloat16)
        fin_out[n, 0, 1] = parts[n, 1, y_next].astype(jnp.bfloat16)
        fin_out[n, 1, 0] = parts[n, 0, y_prev].astype(jnp.bfloat16)
        fin_out[n, 1, 1] = (parts[n, 1, y_prev] + relay_in[n, 1].astype(jnp.float32)).astype(jnp.bfloat16)
        for way in range(2):
            send(fin_out.at[n, way], fin_in.at[n, way], fin_send.at[n, way], fin_recv.at[n, way],
                 dev_y[way]).start()

    def cross(n):
        def summed(dc):
            return parts[n, dc, y] + fin_in[n, 0, dc].astype(jnp.float32) + fin_in[n, 1, dc].astype(jnp.float32)

        for way in range(2):
            wait_in(fin_in.at[n, way], fin_recv.at[n, way])

        @pl.when(n == 0)
        def _():
            for way in range(2):
                wait_in(fin_in.at[LOW, way, 0], fin_recv.at[LOW, way])
                parts[0, 0, y] += fin_in[LOW, way, 0].astype(jnp.float32)

            @pl.when(h == 1)
            def _():
                hx_out[LOW] = low_part(summed(0))
                send(hx_out.at[LOW], hx_in.at[LOW], hx_send.at[LOW], hx_recv.at[LOW], dev_h).start()

        hx_out[n] = summed(1 - h).astype(jnp.bfloat16)
        send(hx_out.at[n], hx_in.at[n], hx_send.at[n], hx_recv.at[n], dev_h).start()
        keep[n] = summed(h)

    lane_row = lax.broadcasted_iota(jnp.int32, (1, VB), 1)

    def energies(n, u, dx):
        wait_in(hx_in.at[n], hx_recv.at[n])

        @pl.when(n == 0)
        def _():
            @pl.when(h == 0)
            def _():
                wait_in(hx_in.at[LOW], hx_recv.at[LOW])
                keep[0] += hx_in[LOW].astype(jnp.float32)

        tile = keep[n] + hx_in[n].astype(jnp.float32)
        first = u % 2 * (z - 1)
        second_row = u // 2 * (3 - 3 * (at_least_two - at_three))
        row_z = z * (1 - (u + 1) // 2) + first + second_row
        row_energy = info_in[(row_z - z + 4) % 4 * 2][1:2, :]
        column_energy = info_in[dx * 8 + h][1:2, :]
        denominator = vsum[...] - row_energy - column_energy
        lane = u * 32 + (h * 4 + dx) * 4

        @pl.when(y < 2)
        def _():
            value = -jnp.sum(tile * (2.0 * tile - tile.T) / denominator, axis=0, keepdims=True)
            value = jnp.sum(value, axis=1, keepdims=True)
            acc[0:1, :] += jnp.where(lane_row == lane + 3 * y, value, 0.0)

        @pl.when(y >= 2)
        def _():
            top, bottom, under = tile[:64], tile[64:], denominator[:64]
            value = -jnp.sum(top * (2.0 * top - bottom) / under, axis=0, keepdims=True)
            other = -jnp.sum(bottom * (2.0 * bottom - top) / under, axis=0, keepdims=True)
            value = jnp.sum(value, axis=1, keepdims=True)
            other = jnp.sum(other, axis=1, keepdims=True)
            acc[0:1, :] += jnp.where(lane_row == lane + 1, value, 0.0) + jnp.where(lane_row == lane + 2, other, 0.0)

    def first_arrivals():
        own_x[0].wait_recv()
        passed_x[0].start()
        own_x[2].wait_recv()
        passed_x[1].start()

    def second_arrivals():
        own_x[1].wait_recv()
        core_copy(3).start()
        own_x[3].wait_recv()
        core_copy(1).start()
        wait_in(panels.at[7], d_recv.at[3])
        wait_in(panels.at[5], d_recv.at[1])

        @pl.when(z >= 1)
        def _():
            wait_in(panels.at[8], z_recv.at[1])

    def third_arrivals():
        for index, (from_z, to_z, u) in enumerate(MOVES):
            if index // 4 == 1:
                @pl.when(z == from_z)
                def _(to_z=to_z, u=u):
                    @pl.when(c == 0)
                    def _():
                        wait_out(panels.at[0], z_send.at[1])
                        pl.semaphore_signal(turn, inc=1, device_id=dev_core, device_id_type=MESH)

                    @pl.when(c == 1)
                    def _():
                        pl.semaphore_wait(turn, 1)
                        z_copy(to_z, u, 1).start()
        passed_x[0].wait_recv()
        passed_x[1].wait_recv()
        core_copy(2).start()
        wait_in(panels.at[6], d_recv.at[2])

    def each(low, high, action):
        def one(n, carry):
            action(n)
            return carry

        lax.fori_loop(low, high, one, 0)

    def step(n, carry):
        u_table, dx_table = carry
        products(n, u_table % 4, dx_table % 4)

        @pl.when(n == 0)
        def _():
            pass_on(0)
            first_arrivals()
            cross(0)
            second_arrivals()

        @pl.when(n == second - 1)
        def _():
            each(1, second, pass_on)
            third_arrivals()

        @pl.when(n == third - 1)
        def _():
            each(second, third, pass_on)

            @pl.when(z <= 2)
            def _():
                wait_in(panels.at[9], z_recv.at[2])

            @pl.when(z == 2)
            def _():
                for to_z in (1, 3):
                    pl.semaphore_signal(calm, inc=1, device_id=(x, to_z, c, y, h), device_id_type=MESH)

        return (u_table // 4, dx_table // 4)

    start = jnp.int32(0)
    lax.fori_loop(0, count, step, (start + by_z(U_TABLE), start + by_z(DX_TABLE)))

    @pl.when(z % 2 == 1)
    def _():
        pl.semaphore_wait(calm, 1)

    each(1, second, cross)
    each(third, count, pass_on)
    each(second, third, cross)
    wait_in(info_in.at[pl.ds(1, NOCC - 1)], tail_recv.at[0])

    def finish(n, carry):
        u_table, dx_table = carry
        energies(n, u_table % 4, dx_table % 4)
        return (u_table // 4, dx_table // 4)

    weights = jnp.zeros((1, VB), jnp.float32)
    for k in range(NOCC):
        weights += info_in[k, 0:1, :]
    each(third, count, cross)
    lax.fori_loop(0, count, finish, (start + by_z(U_TABLE), start + by_z(DX_TABLE)))

    acc[1:2, :] = acc[0:1, :] * weights
    for _, there, device in plane:
        send(acc, first_in.at[there], tail_send.at[1], tail_recv.at[1], device).start()
    first_in[0] = acc[...]
    wait_in(first_in.at[pl.ds(1, 15)], tail_recv.at[1])
    all_out[5:8, :] = jnp.zeros((3, VB), jnp.float32)
    total = jnp.zeros((1, VB), jnp.float32)
    for kx in range(4):
        both = first_in[4 * kx] + first_in[4 * kx + 1] + first_in[4 * kx + 2] + first_in[4 * kx + 3]
        all_out[kx : kx + 1, :] = both[0:1, :]
        total += both[1:2, :]
    all_out[4:5, :] = total
    for _, there, device in column:
        send(all_out, all_in.at[there], tail_send.at[2], tail_recv.at[2], device).start()
    lanes = lax.broadcasted_iota(jnp.int32, (8, VB), 1)
    all_in[0] = all_out[...]

    for k in range(4):
        own_x[k].wait_send()
    for k in range(2):
        passed_x[k].wait_send()
    for dx in range(4):
        core_copy(dx).wait_send()
    wait_out(panels.at[0], z_send.at[0])

    @pl.when(z % 3 == 0)
    def _():
        @pl.when(c == 1)
        def _():
            wait_out(panels.at[0], z_send.at[1])

    def sent(n, carry):
        for k in range(2):
            wait_out(relay_out.at[n, k], relay_send.at[n, k])
            wait_out(fin_out.at[n, k], fin_send.at[n, k])
        wait_out(hx_out.at[n], hx_send.at[n])
        return carry

    lax.fori_loop(0, count, sent, 0)
    wait_out(relay_out.at[LOW, 0], relay_send.at[LOW, 0])
    for way in range(2):
        wait_out(fin_out.at[LOW, way, 0], fin_send.at[LOW, way])

    @pl.when(h == 1)
    def _():
        wait_out(hx_out.at[LOW], hx_send.at[LOW])

    wait_out(info_in.at[pl.ds(1, NOCC - 1)], tail_send.at[0])
    wait_out(first_in.at[pl.ds(1, 15)], tail_send.at[1])

    wait_in(all_in.at[pl.ds(1, 15)], tail_recv.at[2])
    picked = jnp.zeros((8, VB), jnp.float32)
    total = jnp.zeros((1, VB), jnp.float32)
    for kz in range(4):
        for kc in range(2):
            both = all_in[4 * kz + kc] + all_in[4 * kz + 2 + kc]
            total += both[4:5, :]
            for kx in range(4):
                from_row = (xs[kx] * 4 + zs[kz]) * 2 + cs[kc]
                picked += jnp.where(jnp.broadcast_to(wanted, (8, VB)) == from_row * VB + lanes, both[kx : kx + 1, :], 0.0)
    sublane = lax.broadcasted_iota(jnp.int32, (8, VB), 0)
    picked = jnp.sum(picked, axis=1, keepdims=True)
    picked = jnp.sum(jnp.where(sublane == lanes, picked, 0.0), axis=0, keepdims=True)
    out[...] = picked[:, : out.shape[1]]
    total_out[...] = jnp.sum(total, axis=1, keepdims=True)
    wait_out(all_in.at[pl.ds(1, 15)], tail_send.at[2])


def local(b_factors, occ_energies, vir_energies, pair_list, pair_count):
    slot_total = pair_list.shape[1]
    share = slot_total // 8
    vmem = pl.BlockSpec(memory_space=pltpu.VMEM)
    bf16, f32 = jnp.bfloat16, jnp.float32
    dma = pltpu.SemaphoreType.DMA
    tile = (VB, VB)
    pair_energy, total_energy = pl.pallas_call(
        kernel,
        out_shape=(jax.ShapeDtypeStruct((1, share), f32), jax.ShapeDtypeStruct((1, 1), f32)),
        in_specs=[pl.BlockSpec(memory_space=pl.ANY), vmem, vmem, vmem, vmem],
        out_specs=(vmem, vmem),
        scratch_shapes=[
            pltpu.VMEM((10, *b_factors.shape[1:]), bf16),
            pltpu.VMEM((NOCC, 2, VB), f32),
            pltpu.VMEM((NOCC, 2, VB), f32),
            pltpu.VMEM((SLOTS, 2, 4, *tile), f32),
            pltpu.VMEM((SLOTS, 2, *tile), bf16),
            pltpu.VMEM((SLOTS, 2, *tile), bf16),
            pltpu.VMEM((SLOTS, 2, 2, *tile), bf16),
            pltpu.VMEM((SLOTS, 2, 2, *tile), bf16),
            pltpu.VMEM((SLOTS, *tile), f32),
            pltpu.VMEM((SLOTS, *tile), bf16),
            pltpu.VMEM((SLOTS, *tile), bf16),
            pltpu.VMEM(tile, f32),
            pltpu.VMEM((2, VB), f32),
            pltpu.VMEM((16, 2, VB), f32),
            pltpu.VMEM((8, VB), f32),
            pltpu.VMEM((16, 8, VB), f32),
            dma, dma((6,)), dma((6,)), dma((4,)), dma((4,)), dma((2,)), dma((3,)),
            dma((SLOTS, 2)), dma((SLOTS, 2)), dma((SLOTS, 2)), dma((SLOTS, 2)),
            dma((SLOTS,)), dma((SLOTS,)), dma((3,)), dma((3,)), pltpu.SemaphoreType.REGULAR,
            pltpu.SemaphoreType.REGULAR,
        ],
        compiler_params=pltpu.CompilerParams(collective_id=0, has_side_effects=True),
        name="pair_energies",
    )(b_factors, occ_energies.reshape(1, 1), jnp.transpose(pair_list, (2, 0, 1)), pair_count.reshape(1, 1),
      vir_energies.reshape(2, 1, VB))
    return pair_energy, total_energy[0, 0]


def solution(mesh):
    finer = Mesh(mesh.devices.reshape(4, 4, 2, 4, 2), NAMES)
    placed = (P(OCC, None, AUX), P(OCC), P(), P(OCC, None, None), P(OCC))
    return jax.shard_map(
        local, mesh=finer, in_specs=placed, out_specs=(P(OCC, AUX), P()), check_vma=False
    )
```

```python
import jax
import jax.numpy as jnp
from jax import lax
from jax.experimental import pallas as pl
from jax.experimental.pallas import tpu as pltpu
from jax.sharding import Mesh
from jax.sharding import PartitionSpec as P

VB = 128
NV = 256
NOCC = 32
SLOTS = 12
LOW = SLOTS - 1
HALF = 128
OCC = ("occ_0", "occ_1", "occ_2")
AUX = ("aux_0", "aux_1")
NAMES = ("occ_0", "occ_1", "occ_2", "aux_0", "aux_1")
MESH = pl.DeviceIdType.MESH

UNITS = (
    ((0, 0), (0, 1), (0, 2), (2, 0), (2, 1), (2, 3), (2, 2)),
    ((0, 0), (0, 1), (1, 0), (1, 1), (1, 3), (0, 2), (1, 2), (2, 0), (2, 1), (2, 3), (2, 2)),
    ((0, 0), (0, 1), (1, 0), (1, 1), (1, 3), (0, 2), (1, 2), (2, 0), (2, 1), (2, 3), (2, 2)),
    ((0, 0), (0, 1), (1, 0), (1, 1), (1, 3), (0, 2), (1, 2)),
)
COUNT = (7, 11, 11, 7)
SECOND = (2, 5, 5, 5)
THIRD = (3, 7, 7, 7)
MOVES = ((0, 1, 1), (1, 2, 1), (2, 3, 1), (3, 1, 2), (0, 2, 2), (3, 0, 2))
ROW_AT = ((0, 1, 2, -1), (-1, 0, 1, -1), (-1, -1, 0, 1), (2, 2, -1, 0))


def packed(values):
    total = 0
    for place, value in enumerate(values):
        total += value * 4**place
    return total


U_TABLE = tuple(packed([u for u, _ in row]) for row in UNITS)
DX_TABLE = tuple(packed([dx for _, dx in row]) for row in UNITS)


def place_codes(x, z, c, partner, left, right, live):
    partner, left, right = (jnp.maximum(v, 0) for v in (partner, left, right))
    xj, zj, cj = partner >> 3, (partner >> 1) & 3, partner & 1
    xi, zi, ci = (jnp.full(partner.shape, v, jnp.int32) for v in (x, z, c))

    def row_at(first, second):
        key = first * 4 + second
        found = jnp.full(key.shape, -1, jnp.int32)
        for a in range(4):
            for b in range(4):
                if ROW_AT[a][b] >= 0:
                    found = jnp.where(key == a * 4 + b, ROW_AT[a][b], found)
        return found

    direct = row_at(zi, zj)
    ahead = (xj - xi) & 3
    swap = (direct < 0) | ((zi == zj) & (ahead == 3))
    unit = jnp.where(swap, row_at(zj, zi), direct)
    dx = jnp.where(swap, (4 - ahead) & 3, ahead)
    dc = (ci + cj) & 1
    quadrant = jnp.where(swap, right * 2 + left, left * 2 + right)
    device = (jnp.where(swap, xj, xi) * 4 + jnp.where(swap, zi, zj)) * 2 + jnp.where(swap, cj, ci)
    lane = unit * 32 + (dc * 4 + dx) * 4 + quadrant
    return jnp.where(live, device * VB + lane, -1)


def kernel(b_hbm, energy, items, listed, vir, out, total_out, panels, info_out, info_in, parts, relay_out, relay_in, fin_out, fin_in,
           keep, hx_out, hx_in, vsum, sums, spots, acc, first_in, all_out, all_in,
           load_sem, x_send, x_recv, d_send, d_recv, z_send, z_recv, relay_send, relay_recv,
           fin_send, fin_recv, hx_send, hx_recv, tail_send, tail_recv, turn, calm):
    x, z, c, y, h = (lax.axis_index(name) for name in NAMES)
    me = (x * 4 + z) * 2 + c
    xs, zs, ys = ([(v + k) % 4 for k in range(4)] for v in (x, z, y))
    cs, hs = (c, 1 - c), (h, 1 - h)
    at_least_one = (z + 3) // 4
    at_least_two = z // 2
    at_three = z // 3

    def by_z(table):
        steps = [table[k + 1] - table[k] for k in range(3)]
        return table[0] + steps[0] * at_least_one + steps[1] * at_least_two + steps[2] * at_three

    x_next, x_prev, y_next, y_prev = xs[1], xs[3], ys[1], ys[3]
    dev_x = ((x_next, z, c, y, h), (x_prev, z, c, y, h))
    dev_y = ((x, z, c, y_next, h), (x, z, c, y_prev, h))
    dev_core = (x, z, 1 - c, y, h)
    dev_h = (x, z, c, y, 1 - h)

    others = []
    for k in range(1, NOCC):
        kx, kz, kc = k // 8, k // 2 % 4, k % 2
        there = (-kx % 4 * 4 + -kz % 4) * 2 + kc
        others.append((k, there, (xs[kx], zs[kz], cs[kc], y, h), (xs[kx] * 4 + zs[kz]) * 2 + cs[kc]))
    plane = [(k, -(k // 4) % 4 * 4 + -k % 4, (xs[k // 4], z, c, ys[k % 4], h)) for k in range(1, 16)]
    column = [(k, (-(k // 4) % 4 * 2 + k // 2 % 2) * 2 + k % 2, (x, zs[k // 4], cs[k % 2], y, hs[k // 2 % 2]))
              for k in range(1, 16)]
    greeted = [device for _, _, device, _ in others] + [dev_h]
    greeted += [device for k, _, device in plane if k % 4 != 0]
    greeted += [device for k, _, device in column if k // 2 % 2 == 1 and k != 2]

    def send(src, dst, send_sem, recv_sem, device):
        return pltpu.make_async_remote_copy(
            src_ref=src, dst_ref=dst, send_sem=send_sem, recv_sem=recv_sem,
            device_id=device, device_id_type=MESH)

    def wait_in(dst, recv_sem):
        send(dst, dst, x_send.at[0], recv_sem, dev_core).wait_recv()

    def wait_out(src, send_sem):
        send(src, src, send_sem, x_recv.at[0], dev_core).wait_send()

    def half(slot, part):
        return panels.at[slot, pl.ds(part * HALF, HALF)]

    load = pltpu.make_async_copy(b_hbm.at[0], panels.at[0], load_sem)
    load.start()

    barrier = pltpu.get_barrier_semaphore()

    for device in reversed(greeted):
        pl.semaphore_signal(barrier, inc=1, device_id=device, device_id_type=MESH)
    load.wait()
    pl.semaphore_wait(barrier, len(greeted))

    own_x = (
        send(half(0, 0), half(3, 0), x_send.at[0], x_recv.at[0], dev_x[0]),
        send(half(0, 1), half(3, 1), x_send.at[1], x_recv.at[1], dev_x[0]),
        send(half(0, 1), half(1, 1), x_send.at[2], x_recv.at[2], dev_x[1]),
        send(half(0, 0), half(1, 0), x_send.at[3], x_recv.at[3], dev_x[1]),
    )
    passed_x = (
        send(half(3, 0), half(2, 0), x_send.at[4], x_recv.at[4], dev_x[0]),
        send(half(1, 1), half(2, 1), x_send.at[5], x_recv.at[5], dev_x[1]),
    )

    def core_copy(dx):
        return send(panels.at[dx], panels.at[4 + dx], d_send.at[dx], d_recv.at[dx], dev_core)

    def z_copy(to_z, u, kind):
        return send(panels.at[0], panels.at[7 + u], z_send.at[kind], z_recv.at[u], (x, to_z, c, y, h))

    for index, (from_z, to_z, u) in enumerate(MOVES):
        @pl.when(z == from_z)
        def _(to_z=to_z, u=u, kind=index // 4):
            if kind == 0:
                z_copy(to_z, u, kind).start()
            else:
                @pl.when(c == 0)
                def _():
                    z_copy(to_z, u, kind).start()

    own_x[0].start()
    own_x[2].start()
    core_copy(0).start()
    own_x[1].start()
    own_x[3].start()

    slots = items.shape[2]
    slot_of = lax.broadcasted_iota(jnp.int32, (1, slots), 1)
    codes = place_codes(x, z, c, items[0], items[1], items[2], slot_of < listed[...])
    device_hot = lax.broadcasted_iota(jnp.int32, (NOCC, slots), 0) == codes >> 7
    lane_hot = (lax.broadcasted_iota(jnp.int32, (VB, slots), 0) == codes & (VB - 1)) & (codes >= 0)
    hits = lax.dot_general(device_hot.astype(jnp.float32).astype(jnp.bfloat16),
                           lane_hot.astype(jnp.float32).astype(jnp.bfloat16),
                           (((1,), (1,)), ((), ())), preferred_element_type=jnp.float32)
    for k in range(NOCC):
        info_out[k, 0:1, :] = hits[k : k + 1, :]
        info_out[k, 1:2, :] = jnp.broadcast_to(energy[...], (1, VB))
    share = out.shape[1]
    sublane = lax.broadcasted_iota(jnp.int32, (8, slots), 0)
    mine = lax.broadcasted_iota(jnp.int32, (8, slots), 1) == (y * 2 + h) * share + sublane
    wanted = jnp.max(jnp.where(mine & (sublane < share), codes, -1), axis=1, keepdims=True)

    for _, there, device, index in others:
        send(info_out.at[index], info_in.at[there], tail_send.at[0], tail_recv.at[0], device).start()
    info_in[0] = info_out[me]
    sums[...] = jnp.zeros_like(sums)
    spots[...] = jnp.zeros_like(spots)

    wait_in(panels.at[4], d_recv.at[0])

    row_of = lax.broadcasted_iota(jnp.int32, (VB, VB), 0)
    lane_of = lax.broadcasted_iota(jnp.int32, (VB, VB), 1)
    left = vir[0]
    right = vir[1]

    def as_column(row_values, shift):
        wide = jnp.broadcast_to(row_values, (VB, VB))
        return jnp.sum(jnp.where(lane_of == shift, wide, 0.0), axis=1, keepdims=True)

    @pl.when(y == 0)
    def _():
        vsum[...] = as_column(left, row_of) + left

    @pl.when(y == 1)
    def _():
        vsum[...] = as_column(right, row_of) + right

    @pl.when(y == 2)
    def _():
        vsum[...] = as_column(left, row_of % 64) + right

    @pl.when(y == 3)
    def _():
        vsum[...] = as_column(left, row_of % 64 + 64) + right

    count = by_z(COUNT)
    second = by_z(SECOND)
    third = by_z(THIRD)

    def low_part(value):
        return (value - value.astype(jnp.bfloat16).astype(jnp.float32)).astype(jnp.bfloat16)

    def products(n, u, dx):
        row_slot = (7 + u) * ((u + 3) // 4)
        rows = panels[row_slot]
        for dc in range(2):
            block = lax.dot_general(rows, panels[dc * 4 + dx], (((1,), (1,)), ((), ())),
                                    preferred_element_type=jnp.float32)
            upper = block[:VB, VB:]
            lower = block[VB:, :VB].T
            parts[n, dc, 0] = block[:VB, :VB]
            parts[n, dc, 1] = block[VB:, VB:]
            parts[n, dc, 2, 0:64] = upper[:64]
            parts[n, dc, 2, 64:128] = lower[:64]
            parts[n, dc, 3, 0:64] = upper[64:]
            parts[n, dc, 3, 64:128] = lower[64:]
        far = ys[2]
        for dc in range(2):
            relay_out[n, dc] = parts[n, dc, far].astype(jnp.bfloat16)
            send(relay_out.at[n, dc], relay_in.at[n, dc], relay_send.at[n, dc], relay_recv.at[n, dc],
                 dev_y[dc]).start()

        @pl.when(n == 0)
        def _():
            relay_out[LOW, 0] = low_part(parts[0, 0, far])
            send(relay_out.at[LOW, 0], relay_in.at[LOW, 0], relay_send.at[LOW, 0], relay_recv.at[LOW, 0],
                 dev_y[0]).start()

    def pass_on_low():
        wait_in(relay_in.at[LOW, 0], relay_recv.at[LOW, 0])
        parts[0, 0, y_next] += relay_in[LOW, 0].astype(jnp.float32)
        fin_out[LOW, 0, 0] = low_part(parts[0, 0, y_next] + relay_in[0, 0].astype(jnp.float32))
        fin_out[LOW, 1, 0] = low_part(parts[0, 0, y_prev])
        for way in range(2):
            send(fin_out.at[LOW, way, 0], fin_in.at[LOW, way, 0], fin_send.at[LOW, way], fin_recv.at[LOW, way],
                 dev_y[way]).start()

    def pass_on(n):
        for dc in range(2):
            wait_in(relay_in.at[n, dc], relay_recv.at[n, dc])

        @pl.when(n == 0)
        def _():
            pass_on_low()

        fin_out[n, 0, 0] = (parts[n, 0, y_next] + relay_in[n, 0].astype(jnp.float32)).astype(jnp.bfloat16)
        fin_out[n, 0, 1] = parts[n, 1, y_next].astype(jnp.bfloat16)
        fin_out[n, 1, 0] = parts[n, 0, y_prev].astype(jnp.bfloat16)
        fin_out[n, 1, 1] = (parts[n, 1, y_prev] + relay_in[n, 1].astype(jnp.float32)).astype(jnp.bfloat16)
        for way in range(2):
            send(fin_out.at[n, way], fin_in.at[n, way], fin_send.at[n, way], fin_recv.at[n, way],
                 dev_y[way]).start()

    def cross(n):
        def summed(dc):
            return parts[n, dc, y] + fin_in[n, 0, dc].astype(jnp.float32) + fin_in[n, 1, dc].astype(jnp.float32)

        for way in range(2):
            wait_in(fin_in.at[n, way], fin_recv.at[n, way])

        @pl.when(n == 0)
        def _():
            for way in range(2):
                wait_in(fin_in.at[LOW, way, 0], fin_recv.at[LOW, way])
                parts[0, 0, y] += fin_in[LOW, way, 0].astype(jnp.float32)

            @pl.when(h == 1)
            def _():
                hx_out[LOW] = low_part(summed(0))
                send(hx_out.at[LOW], hx_in.at[LOW], hx_send.at[LOW], hx_recv.at[LOW], dev_h).start()

        hx_out[n] = summed(1 - h).astype(jnp.bfloat16)
        send(hx_out.at[n], hx_in.at[n], hx_send.at[n], hx_recv.at[n], dev_h).start()
        keep[n] = summed(h)

    lane_row = lax.broadcasted_iota(jnp.int32, (1, VB), 1)

    def energies(n, u, dx):
        wait_in(hx_in.at[n], hx_recv.at[n])

        @pl.when(n == 0)
        def _():
            @pl.when(h == 0)
            def _():
                wait_in(hx_in.at[LOW], hx_recv.at[LOW])
                keep[0] += hx_in[LOW].astype(jnp.float32)

        tile = keep[n] + hx_in[n].astype(jnp.float32)
        first = u % 2 * (z - 1)
        second_row = u // 2 * (3 - 3 * (at_least_two - at_three))
        row_z = z * (1 - (u + 1) // 2) + first + second_row
        row_energy = info_in[(row_z - z + 4) % 4 * 2][1:2, :]
        column_energy = info_in[dx * 8 + h][1:2, :]
        denominator = vsum[...] - row_energy - column_energy
        lane = u * 32 + (h * 4 + dx) * 4

        @pl.when(y < 2)
        def _():
            value = -jnp.sum(tile * (2.0 * tile - tile.T) / denominator, axis=0, keepdims=True)
            sums[pl.ds(n, 1), :] = value
            spots[pl.ds(n, 1), :] = jnp.where(lane_row == lane + 3 * y, 1.0, 0.0)

        @pl.when(y >= 2)
        def _():
            top, bottom, under = tile[:64], tile[64:], denominator[:64]
            value = -jnp.sum(top * (2.0 * top - bottom) / under, axis=0, keepdims=True)
            other = -jnp.sum(bottom * (2.0 * bottom - top) / under, axis=0, keepdims=True)
            sums[pl.ds(n, 1), :] = value
            sums[pl.ds(n + SLOTS, 1), :] = other
            spots[pl.ds(n, 1), :] = jnp.where(lane_row == lane + 1, 1.0, 0.0)
            spots[pl.ds(n + SLOTS, 1), :] = jnp.where(lane_row == lane + 2, 1.0, 0.0)

    def first_arrivals():
        own_x[0].wait_recv()
        passed_x[0].start()
        own_x[2].wait_recv()
        passed_x[1].start()

    def second_arrivals():
        own_x[1].wait_recv()
        core_copy(3).start()
        own_x[3].wait_recv()
        core_copy(1).start()
        wait_in(panels.at[7], d_recv.at[3])
        wait_in(panels.at[5], d_recv.at[1])

        @pl.when(z >= 1)
        def _():
            wait_in(panels.at[8], z_recv.at[1])

    def third_arrivals():
        for index, (from_z, to_z, u) in enumerate(MOVES):
            if index // 4 == 1:
                @pl.when(z == from_z)
                def _(to_z=to_z, u=u):
                    @pl.when(c == 0)
                    def _():
                        wait_out(panels.at[0], z_send.at[1])
                        pl.semaphore_signal(turn, inc=1, device_id=dev_core, device_id_type=MESH)

                    @pl.when(c == 1)
                    def _():
                        pl.semaphore_wait(turn, 1)
                        z_copy(to_z, u, 1).start()
        passed_x[0].wait_recv()
        passed_x[1].wait_recv()
        core_copy(2).start()
        wait_in(panels.at[6], d_recv.at[2])

    def each(low, high, action):
        def one(n, carry):
            action(n)
            return carry

        lax.fori_loop(low, high, one, 0)

    def step(n, carry):
        u_table, dx_table = carry
        products(n, u_table % 4, dx_table % 4)

        @pl.when(n == 0)
        def _():
            pass_on(0)
            first_arrivals()
            cross(0)
            second_arrivals()

        @pl.when(n == second - 1)
        def _():
            each(1, second, pass_on)
            third_arrivals()

        @pl.when(n == third - 1)
        def _():
            each(second, third, pass_on)

            @pl.when(z <= 2)
            def _():
                wait_in(panels.at[9], z_recv.at[2])

            @pl.when(z == 2)
            def _():
                for to_z in (1, 3):
                    pl.semaphore_signal(calm, inc=1, device_id=(x, to_z, c, y, h), device_id_type=MESH)

        return (u_table // 4, dx_table // 4)

    start = jnp.int32(0)
    lax.fori_loop(0, count, step, (start + by_z(U_TABLE), start + by_z(DX_TABLE)))

    @pl.when(z % 2 == 1)
    def _():
        pl.semaphore_wait(calm, 1)

    each(1, second, cross)
    each(third, count, pass_on)
    each(second, third, cross)
    wait_in(info_in.at[pl.ds(1, NOCC - 1)], tail_recv.at[0])

    def finish(n, carry):
        u_table, dx_table = carry
        energies(n, u_table % 4, dx_table % 4)
        return (u_table // 4, dx_table // 4)

    weights = jnp.zeros((1, VB), jnp.float32)
    for k in range(NOCC):
        weights += info_in[k, 0:1, :]
    each(third, count, cross)
    lax.fori_loop(0, count, finish, (start + by_z(U_TABLE), start + by_z(DX_TABLE)))

    values = jnp.sum(sums[...], axis=1, keepdims=True)
    found = jnp.sum(spots[...] * values, axis=0, keepdims=True)
    acc[0:1, :] = found
    acc[1:2, :] = found * weights
    for _, there, device in plane:
        send(acc, first_in.at[there], tail_send.at[1], tail_recv.at[1], device).start()
    first_in[0] = acc[...]
    wait_in(first_in.at[pl.ds(1, 15)], tail_recv.at[1])
    all_out[5:8, :] = jnp.zeros((3, VB), jnp.float32)
    total = jnp.zeros((1, VB), jnp.float32)
    for kx in range(4):
        both = first_in[4 * kx] + first_in[4 * kx + 1] + first_in[4 * kx + 2] + first_in[4 * kx + 3]
        all_out[kx : kx + 1, :] = both[0:1, :]
        total += both[1:2, :]
    all_out[4:5, :] = total
    for _, there, device in column:
        send(all_out, all_in.at[there], tail_send.at[2], tail_recv.at[2], device).start()
    lanes = lax.broadcasted_iota(jnp.int32, (8, VB), 1)
    all_in[0] = all_out[...]

    for k in range(4):
        own_x[k].wait_send()
    for k in range(2):
        passed_x[k].wait_send()
    for dx in range(4):
        core_copy(dx).wait_send()
    wait_out(panels.at[0], z_send.at[0])

    @pl.when(z % 3 == 0)
    def _():
        @pl.when(c == 1)
        def _():
            wait_out(panels.at[0], z_send.at[1])

    def sent(n, carry):
        for k in range(2):
            wait_out(relay_out.at[n, k], relay_send.at[n, k])
            wait_out(fin_out.at[n, k], fin_send.at[n, k])
        wait_out(hx_out.at[n], hx_send.at[n])
        return carry

    lax.fori_loop(0, count, sent, 0)
    wait_out(relay_out.at[LOW, 0], relay_send.at[LOW, 0])
    for way in range(2):
        wait_out(fin_out.at[LOW, way, 0], fin_send.at[LOW, way])

    @pl.when(h == 1)
    def _():
        wait_out(hx_out.at[LOW], hx_send.at[LOW])

    wait_out(info_in.at[pl.ds(1, NOCC - 1)], tail_send.at[0])
    wait_out(first_in.at[pl.ds(1, 15)], tail_send.at[1])

    wait_in(all_in.at[pl.ds(1, 15)], tail_recv.at[2])
    picked = jnp.zeros((8, VB), jnp.float32)
    total = jnp.zeros((1, VB), jnp.float32)
    for kz in range(4):
        for kc in range(2):
            both = all_in[4 * kz + kc] + all_in[4 * kz + 2 + kc]
            total += both[4:5, :]
            for kx in range(4):
                from_row = (xs[kx] * 4 + zs[kz]) * 2 + cs[kc]
                picked += jnp.where(jnp.broadcast_to(wanted, (8, VB)) == from_row * VB + lanes, both[kx : kx + 1, :], 0.0)
    sublane = lax.broadcasted_iota(jnp.int32, (8, VB), 0)
    picked = jnp.sum(picked, axis=1, keepdims=True)
    picked = jnp.sum(jnp.where(sublane == lanes, picked, 0.0), axis=0, keepdims=True)
    out[...] = picked[:, : out.shape[1]]
    total_out[...] = jnp.sum(total, axis=1, keepdims=True)
    wait_out(all_in.at[pl.ds(1, 15)], tail_send.at[2])


def local(b_factors, occ_energies, vir_energies, pair_list, pair_count):
    slot_total = pair_list.shape[1]
    share = slot_total // 8
    vmem = pl.BlockSpec(memory_space=pltpu.VMEM)
    bf16, f32 = jnp.bfloat16, jnp.float32
    dma = pltpu.SemaphoreType.DMA
    tile = (VB, VB)
    pair_energy, total_energy = pl.pallas_call(
        kernel,
        out_shape=(jax.ShapeDtypeStruct((1, share), f32), jax.ShapeDtypeStruct((1, 1), f32)),
        in_specs=[pl.BlockSpec(memory_space=pl.ANY), vmem, vmem, vmem, vmem],
        out_specs=(vmem, vmem),
        scratch_shapes=[
            pltpu.VMEM((10, *b_factors.shape[1:]), bf16),
            pltpu.VMEM((NOCC, 2, VB), f32),
            pltpu.VMEM((NOCC, 2, VB), f32),
            pltpu.VMEM((SLOTS, 2, 4, *tile), f32),
            pltpu.VMEM((SLOTS, 2, *tile), bf16),
            pltpu.VMEM((SLOTS, 2, *tile), bf16),
            pltpu.VMEM((SLOTS, 2, 2, *tile), bf16),
            pltpu.VMEM((SLOTS, 2, 2, *tile), bf16),
            pltpu.VMEM((SLOTS, *tile), f32),
            pltpu.VMEM((SLOTS, *tile), bf16),
            pltpu.VMEM((SLOTS, *tile), bf16),
            pltpu.VMEM(tile, f32),
            pltpu.VMEM((2 * SLOTS, VB), f32),
            pltpu.VMEM((2 * SLOTS, VB), f32),
            pltpu.VMEM((2, VB), f32),
            pltpu.VMEM((16, 2, VB), f32),
            pltpu.VMEM((8, VB), f32),
            pltpu.VMEM((16, 8, VB), f32),
            dma, dma((6,)), dma((6,)), dma((4,)), dma((4,)), dma((2,)), dma((3,)),
            dma((SLOTS, 2)), dma((SLOTS, 2)), dma((SLOTS, 2)), dma((SLOTS, 2)),
            dma((SLOTS,)), dma((SLOTS,)), dma((3,)), dma((3,)), pltpu.SemaphoreType.REGULAR,
            pltpu.SemaphoreType.REGULAR,
        ],
        compiler_params=pltpu.CompilerParams(collective_id=0, has_side_effects=True),
        name="pair_energies",
    )(b_factors, occ_energies.reshape(1, 1), jnp.transpose(pair_list, (2, 0, 1)), pair_count.reshape(1, 1),
      vir_energies.reshape(2, 1, VB))
    return pair_energy, total_energy[0, 0]


def solution(mesh):
    finer = Mesh(mesh.devices.reshape(4, 4, 2, 4, 2), NAMES)
    placed = (P(OCC, None, AUX), P(OCC), P(), P(OCC, None, None), P(OCC))
    return jax.shard_map(
        local, mesh=finer, in_specs=placed, out_specs=(P(OCC, AUX), P()), check_vma=False
    )
```
